256 devices in a mesh: face: 8 (over z_hi, x), patch: 32 (over z_lo, y, core).
Axes of the slice: x: 4, y: 4, z: 8 (z_hi: 2, z_lo: 4; z = z_hi * 4 + z_lo), core: 2. Of those that a mesh axis runs over, the one named last changes fastest.
Arguments:
- features: bfloat16 [32, 8, 131072], P(None, 'face', 'patch'), may hold values from -6 to 6
- film_first: float32 [2, 32], replicated, may hold values from -3 to 3
- weight_first: bfloat16 [32, 288], replicated, may hold values from -0.375 to 0.375
- film_second: float32 [2, 32], replicated, may hold values from -3 to 3
- weight_second: bfloat16 [64, 288], replicated, may hold values from -0.375 to 0.375
- film_third: float32 [2, 64], replicated, may hold values from -3 to 3
- weight_third: bfloat16 [128, 576], replicated, may hold values from -0.25 to 0.25
- film_fourth: float32 [2, 128], replicated, may hold values from -3 to 3
- weight_fourth: bfloat16 [128, 1152], replicated, may hold values from -0.1875 to 0.1875
- film_fifth: float32 [2, 192], replicated, may hold values from -3 to 3
- weight_fifth: bfloat16 [64, 1728], replicated, may hold values from -0.15625 to 0.15625
- film_sixth: float32 [2, 96], replicated, may hold values from -3 to 3
- weight_sixth: bfloat16 [32, 864], replicated, may hold values from -0.21875 to 0.21875
- link_patch: int32 [8, 32, 8], replicated, may hold values from 0 to 31, as said below
- link_shift: int32 [8, 32, 8], replicated, may hold values from -1 to 1, as said below
- link_turn: int32 [8, 32, 8], replicated, may hold values from 0 to 3, as said below
Outputs:
- denoised: bfloat16 [32, 8, 131072], P(None, 'face', 'patch')
The draws below stay inside these ranges and needn't reach their ends.
Inputs may be any that keep to these rules, and one draw needn't show every extreme that they name: `link_patch`: patch p of a face sits at row p // 8 and column p % 8 of a 4 x 8 grid of patches. For a direction that stays inside that grid the entry is the grid neighbour. For a direction that leaves it the entry is a patch on the outer row or column of the neighbouring face's grid such that every cell that padded reads from it lies on that face's outer border. `link_shift`: 0 for a direction that stays inside the face's grid of patches, -1 or +1 for one that leaves it. `link_turn`: 0 for a direction that stays inside the face's grid of patches.
All inputs are finite; a program needn't handle non-finite values.
Results may differ from the reference program's by a relative error of at most 0.009.
Values may be sent and summed in bfloat16 or wider, within the bound.
No kernel may reach another device: no remote copies, remote signals or barrier semaphores. Data moves between devices by JAX's collectives and lax.ppermute only.
A program may use at most 128 MiB of HBM per device.

```python
import math
import jax
import jax.numpy as jnp
from jax import lax

C1 = 32
C2 = 64
C3 = 128
PATCH_ROWS = 4
PATCH_COLS = 8
CELLS = 4096
N_FACE = 8
N_PATCH = 32


def link_tables(key):
    table_shape = (N_FACE, N_PATCH, 8)
    patch_ids = jnp.arange(N_PATCH, dtype=jnp.int32)[None, :, None]
    patch_row = patch_ids // PATCH_COLS
    patch_col = patch_ids % PATCH_COLS
    step_row = jnp.array([-1, 1, 0, 0, -1, -1, 1, 1], dtype=jnp.int32)[None, None, :]
    step_col = jnp.array([0, 0, -1, 1, -1, 1, -1, 1], dtype=jnp.int32)[None, None, :]
    near_row = patch_row + step_row
    near_col = patch_col + step_col
    inside = (near_row >= 0) & (near_row < PATCH_ROWS) & (near_col >= 0) & (near_col < PATCH_COLS)
    inside = jnp.broadcast_to(inside, table_shape)
    grid_patch = jnp.broadcast_to(near_row * PATCH_COLS + near_col, table_shape)
    far_side = jax.random.randint(jax.random.fold_in(key, 202), table_shape, 0, 2, dtype=jnp.int32) * 2 - 1
    far_turn = jax.random.randint(jax.random.fold_in(key, 303), table_shape, 0, 4, dtype=jnp.int32)
    read_edge = jnp.broadcast_to(jnp.array([1, 0, 3, 2, 1, 1, 0, 0], dtype=jnp.int32)[None, None, :], table_shape)
    source_of = jnp.array([3, 2, 0, 1], dtype=jnp.int32)
    edge_now = read_edge
    for count in range(1, 4):
        edge_now = jnp.where(far_turn >= count, source_of[edge_now], edge_now)
    pick_row = jax.random.randint(jax.random.fold_in(key, 404), table_shape, 0, PATCH_ROWS, dtype=jnp.int32)
    pick_col = jax.random.randint(jax.random.fold_in(key, 505), table_shape, 0, PATCH_COLS, dtype=jnp.int32)
    far_patch = jnp.where(edge_now == 0, pick_col, jnp.where(edge_now == 1, (PATCH_ROWS - 1) * PATCH_COLS + pick_col, jnp.where(edge_now == 2, pick_row * PATCH_COLS, pick_row * PATCH_COLS + PATCH_COLS - 1)))
    zeros_table = jnp.zeros(table_shape, jnp.int32)
    return (jnp.where(inside, grid_patch, far_patch).astype(jnp.int32), jnp.where(inside, zeros_table, far_side).astype(jnp.int32), jnp.where(inside, zeros_table, far_turn).astype(jnp.int32))


def draw_link_patch(key, part):
    return link_tables(key)[0]


def draw_link_shift(key, part):
    return link_tables(key)[1]


def draw_link_turn(key, part):
    return link_tables(key)[2]


def shard_levels(key, dims, cuts, least, top_value):
    def one(dim, parts):
        draws = jax.random.uniform(jax.random.fold_in(jax.random.fold_in(key, 6), dim), (parts,), jnp.float32, least / len(cuts), top_value / len(cuts))
        return jnp.repeat(jnp.exp(draws), dims[dim] // parts).reshape((-1,) + (1,) * (len(dims) - dim - 1))

    level = one(*cuts[0])
    for cut in cuts[1:]:
        level = level * one(*cut)
    return level


def noise(own_key, shape, spread, limit, split=(), kind=jnp.bfloat16):
    level = shard_levels(own_key, shape, split, -0.22, 0.18) if split else 1.0
    values = jax.random.normal(own_key, shape, jnp.float32) * spread * level
    return jnp.minimum(jnp.maximum(values, -limit), limit).astype(kind)


def setup_inputs(seed: int = 0) -> dict:
    seeds = jax.random.split(jax.random.key(seed), 17)
    return {
        "features": noise(seeds[0], (C1, N_FACE, N_PATCH * CELLS), 1.0, 6.0, ((1, 8), (2, 32))),
        "film_first": noise(seeds[1], (2, C1), 0.5, 3.0, (), jnp.float32),
        "weight_first": noise(seeds[2], (C1, 9 * C1), (9 * C1) ** -0.5, 0.375),
        "film_second": noise(seeds[3], (2, C1), 0.5, 3.0, (), jnp.float32),
        "weight_second": noise(seeds[4], (C2, 9 * C1), (9 * C1) ** -0.5, 0.375),
        "film_third": noise(seeds[5], (2, C2), 0.5, 3.0, (), jnp.float32),
        "weight_third": noise(seeds[6], (C3, 9 * C2), (9 * C2) ** -0.5, 0.25),
        "film_fourth": noise(seeds[7], (2, C3), 0.5, 3.0, (), jnp.float32),
        "weight_fourth": noise(seeds[8], (C3, 9 * C3), (9 * C3) ** -0.5, 0.1875),
        "film_fifth": noise(seeds[9], (2, C3 + C2), 0.5, 3.0, (), jnp.float32),
        "weight_fifth": noise(seeds[10], (C2, 9 * (C3 + C2)), (9 * (C3 + C2)) ** -0.5, 0.15625),
        "film_sixth": noise(seeds[11], (2, C2 + C1), 0.5, 3.0, (), jnp.float32),
        "weight_sixth": noise(seeds[12], (C1, 9 * (C2 + C1)), (9 * (C2 + C1)) ** -0.5, 0.21875),
        "link_patch": draw_link_patch(jax.random.fold_in(seeds[16], 71), 0),
        "link_shift": draw_link_shift(jax.random.fold_in(seeds[16], 71), 0),
        "link_turn": draw_link_turn(jax.random.fold_in(seeds[16], 71), 0),
    }


EPSILON = 1e-05
FLOOR_SQUARE = 0.5

def activate(values, modulation):
    channels = values.shape[-2]
    mean_square = lax.optimization_barrier(jnp.mean(values * values, axis=-2, keepdims=True))
    if channels >= 64:
        inverse = lax.rsqrt(mean_square + EPSILON)
    else:
        inverse = lax.rsqrt(jnp.maximum(mean_square, FLOOR_SQUARE))
    shaped = values * inverse * (1.0 + modulation[0][:, None]) + modulation[1][:, None]
    return jax.nn.silu(shaped).astype(jnp.bfloat16)

def frame_of(grids):
    return jnp.stack([grids[..., 0, :], grids[..., -1, :], grids[..., :, 0], grids[..., :, -1]], axis=-3)

def turn_once(frames):
    return jnp.stack([frames[..., 3, :, :], frames[..., 2, :, :], frames[..., 0, :, ::-1], frames[..., 1, :, ::-1]], axis=-3)

def turned(frames, quarters):
    result = frames
    current = frames
    for count in range(1, 4):
        current = turn_once(current)
        result = jnp.where((quarters == count)[:, None, None, None], current, result)
    return result

def cycle_of(frames):
    edges = jnp.stack([frames[0, 1], frames[1, 0], frames[2, 3], frames[3, 2]])
    corners = jnp.stack([frames[4, 1, :, -1], frames[5, 1, :, 0], frames[6, 0, :, -1], frames[7, 0, :, 0]])
    return (edges, corners)

def assemble(grid, edges, corners):
    middle = jnp.concatenate([edges[2][:, :, None], grid, edges[3][:, :, None]], axis=2)
    upper = jnp.concatenate([corners[0][:, None], edges[0], corners[1][:, None]], axis=1)
    lowest = jnp.concatenate([corners[2][:, None], edges[1], corners[3][:, None]], axis=1)
    return jnp.concatenate([upper[:, None, :], middle, lowest[:, None, :]], axis=1)

def stencil(padded, weight):
    channels = padded.shape[0]
    length = padded.shape[1] - 2
    columns = [padded[:, row_start:row_start + length, col_start:col_start + length].reshape(channels, length * length) for row_start in range(3) for col_start in range(3)]
    return jnp.dot(weight, jnp.concatenate(columns, axis=0), preferred_element_type=jnp.float32)

def level_conv(active, weight, tables):
    link_patch, link_shift, link_turn = tables
    face_count, patch_count, channels, cells = active.shape
    length = math.isqrt(cells)
    grids = active.reshape(face_count, patch_count, channels, length, length)
    frames = frame_of(grids)

    def one_patch(position):
        face_id = position // patch_count
        patch_id = position % patch_count
        source_face = jnp.mod(face_id + link_shift[face_id, patch_id], face_count)
        neighbours = frames[source_face, link_patch[face_id, patch_id]]
        edges, corners = cycle_of(turned(neighbours, link_turn[face_id, patch_id]))
        return stencil(assemble(grids[face_id, patch_id], edges, corners), weight)
    result = lax.map(one_patch, jnp.arange(face_count * patch_count, dtype=jnp.int32))
    return result.reshape(face_count, patch_count, weight.shape[0], cells)

def coarsen(field):
    leading = field.shape[:-1]
    length = math.isqrt(field.shape[-1])
    half_side = length // 2
    blocks = field.reshape(leading + (half_side, 2, half_side, 2))
    return lax.optimization_barrier(jnp.mean(blocks, axis=(-3, -1))).reshape(leading + (half_side * half_side,))

def refine(field):
    leading = field.shape[:-1]
    length = math.isqrt(field.shape[-1])
    grid = field.reshape(leading + (length, length))
    grid = jnp.repeat(jnp.repeat(grid, 2, axis=-2), 2, axis=-1)
    return grid.reshape(leading + (4 * length * length,))

def reference(features, film_first, weight_first, film_second, weight_second, film_third, weight_third, film_fourth, weight_fourth, film_fifth, weight_fifth, film_sixth, weight_sixth, link_patch, link_shift, link_turn):
    tables = (link_patch, link_shift, link_turn)
    fine = features.reshape(C1, N_FACE, N_PATCH, CELLS).transpose(1, 2, 0, 3).astype(jnp.float32)
    first = fine + level_conv(activate(fine, film_first), weight_first, tables)
    skip_fine = first.astype(jnp.bfloat16)
    second = level_conv(activate(coarsen(first), film_second), weight_second, tables)
    skip_middle = second.astype(jnp.bfloat16)
    third = level_conv(activate(coarsen(second), film_third), weight_third, tables)
    fourth = third + level_conv(activate(third, film_fourth), weight_fourth, tables)
    joined_middle = jnp.concatenate([refine(fourth), skip_middle.astype(jnp.float32)], axis=-2)
    fifth = level_conv(activate(joined_middle, film_fifth), weight_fifth, tables)
    joined_fine = jnp.concatenate([refine(fifth), skip_fine.astype(jnp.float32)], axis=-2)
    result = skip_fine.astype(jnp.float32) + level_conv(activate(joined_fine, film_sixth), weight_sixth, tables)
    result = result.astype(jnp.bfloat16)
    return result.transpose(2, 0, 1, 3).reshape(C1, N_FACE, N_PATCH * CELLS)
```

```python
import functools

import jax
import jax.numpy as jnp
import numpy as np
from jax import lax
from jax.experimental import pallas as pl
from jax.experimental.pallas import tpu as pltpu
from jax.sharding import PartitionSpec as P

EPSILON = 1e-05
FLOOR_SQUARE = 0.5
F32 = jnp.float32
BF16 = jnp.bfloat16
TAPS = [(u, v) for u in (-1, 0, 1) for v in (-1, 0, 1)]
FILM_ROWS = {1: (0, 32), 2: (32, 64), 3: (64, 128), 4: (128, 256), 5: (256, 448), 6: (448, 544)}
TURN_EDGE = np.array([[0, 1, 2, 3], [3, 2, 0, 1], [1, 0, 3, 2], [2, 3, 1, 0]])
TURN_FLIP = np.array([[0, 0, 0, 0], [0, 0, 1, 1], [1, 1, 1, 1], [1, 1, 0, 0]])
READ_EDGE = np.array([1, 0, 3, 2, 1, 1, 0, 0])
READ_END = np.array([0, 0, 0, 0, 1, 0, 1, 0])
CORNERS = [(4, 0), (5, 1), (6, 2), (7, 3)]
BLOCKS = {
    64: [[(0, 0), (1, 64)], [(2, 0), (3, 64)], CORNERS],
    32: [[(0, 0), (1, 32), (2, 64), (3, 96)], CORNERS],
    16: [[(0, 0), (1, 16), (2, 32), (3, 48), (4, 64), (5, 65), (6, 66), (7, 67)]],
}


def dot(a, b):
    return jnp.dot(a, b, preferred_element_type=F32)


def lanes_of(width):
    return lax.broadcasted_iota(jnp.int32, (1, width), 1)


def halves(x):
    high = x.astype(BF16)
    return high, (x - high.astype(F32)).astype(BF16)


def activate(values, film):
    mean_square = jnp.mean(values * values, axis=0, keepdims=True)
    if values.shape[0] >= 64:
        inverse = lax.rsqrt(mean_square + EPSILON)
    else:
        inverse = lax.rsqrt(jnp.maximum(mean_square, FLOOR_SQUARE))
    shaped = values * inverse * (1.0 + film[:, 0:1]) + film[:, 1:2]
    return (shaped / (1.0 + jnp.exp(-shaped))).astype(BF16)


def film_of(ref, index):
    first, last = FILM_ROWS[index]
    return ref[first:last, :]


def by_chunks(x, matrix):
    channels = x.shape[0]
    run = matrix.shape[0]
    count = x.shape[1] // run
    stacked = jnp.concatenate([x[:, run * k : run * (k + 1)] for k in range(count)], axis=0)
    high, low = halves(stacked)
    result = dot(high, matrix) + dot(low, matrix)
    return jnp.concatenate([result[channels * k : channels * (k + 1)] for k in range(count)], axis=1)


def frame_64(a, west_east_t):
    cells = a.shape[1]
    upper = jnp.where(lanes_of(128) < 64, a[:, :128].astype(F32), a[:, cells - 128 :].astype(F32))
    return jnp.concatenate([upper, dot(a, west_east_t)], axis=0).astype(BF16)


def frame_16(a, low_t, high_t):
    half = a.shape[0] // 2
    return (dot(a[:half], low_t) + dot(a[half:], high_t)).astype(BF16)


def halo_of(own, down, up, first, channels, blocks):
    rows = slice(first, first + channels * blocks)
    packed = own[rows, :].astype(F32) + down[rows, :].astype(F32) + up[rows, :].astype(F32)
    return jnp.concatenate([packed[channels * k : channels * (k + 1)] for k in range(blocks)], axis=1)


def expand(z, matrix):
    high, low = halves(z)
    both = dot(jnp.concatenate([high, low], axis=0), matrix)
    return both[: z.shape[0]] + both[z.shape[0] :]


def border_sums(halo, weight, length):
    products = dot(weight, halo)
    out_channels = weight.shape[0] // 9
    width = halo.shape[1]

    def tap(u, v):
        t = 3 * (u + 1) + v + 1
        return products[t * out_channels : (t + 1) * out_channels]

    lane = lanes_of(width)
    part = lane // length
    place = lane % length

    def along(step):
        return jnp.where(
            part == 0,
            tap(-1, step),
            jnp.where(part == 1, tap(1, step), jnp.where(part == 2, tap(step, -1), tap(step, 1))),
        )

    end = 4 * length
    corner = jnp.where(lane == end, tap(-1, -1), 0.0)
    corner = jnp.where(lane == end + 1, tap(-1, 1), corner)
    corner = jnp.where(lane == end + 2, tap(1, -1), corner)
    corner = jnp.where(lane == end + 3, tap(1, 1), corner)
    edge = part < 4
    before = jnp.where(edge & (place != 0), pltpu.roll(along(-1), 1, 1), 0.0)
    after = jnp.where(edge & (place != length - 1), pltpu.roll(along(1), width - 1, 1), 0.0)
    return jnp.where(edge, along(0), corner) + before + after


def with_halo_64(base, halo, weight, west_east, corner_map):
    sums = border_sums(halo, weight, 64)
    rows = sums[:, :128] + expand(sums[:, 256:], corner_map)
    total = base + expand(sums[:, 128:256], west_east)
    cells = total.shape[1]
    low = lanes_of(128) < 64
    top = total[:, :128] + jnp.where(low, rows, 0.0)
    bottom = total[:, cells - 128 :] + jnp.where(low, 0.0, rows)
    return jnp.concatenate([top, total[:, 128 : cells - 128], bottom], axis=1)


def with_halo(base, halo, weight, length, matrix):
    return base + expand(border_sums(halo, weight, length), matrix)


def main_kernel(a_ref, w_ref, out_ref, products, *, length):
    products[...] = dot(w_ref[...], a_ref[...])
    out_channels, cells = out_ref.shape
    lane = lanes_of(cells)
    place = lane % length

    def tap(u, v):
        t = 3 * (u + 1) + v + 1
        return products[t * out_channels : (t + 1) * out_channels, :]

    def column(v):
        above = jnp.where(lane < length, 0.0, pltpu.roll(tap(-1, v), length, 1))
        below = jnp.where(lane >= cells - length, 0.0, pltpu.roll(tap(1, v), cells - length, 1))
        return tap(0, v) + above + below

    total = column(0)
    total += jnp.where(place == 0, 0.0, pltpu.roll(column(-1), 1, 1))
    total += jnp.where(place == length - 1, 0.0, pltpu.roll(column(1), cells - 1, 1))
    out_ref[...] = total


def main_conv(a, weight, length):
    taps_out = weight.shape[0]
    cells = a.shape[1]
    return pl.pallas_call(
        functools.partial(main_kernel, length=length),
        out_shape=jax.ShapeDtypeStruct((taps_out // 9, cells), F32),
        scratch_shapes=[pltpu.VMEM((taps_out, cells), F32)],
        cost_estimate=pl.CostEstimate(
            flops=2 * taps_out * weight.shape[1] * cells * 8, bytes_accessed=a.size * 2 + taps_out * cells, transcendentals=0
        ),
        name="main_conv",
    )(a, weight)


def pick_kernel(code_ref, gathered, own_ref, up_ref, down_ref, *, specs):
    for target, (out, wanted) in enumerate(((own_ref, 1), (up_ref, 0), (down_ref, 2))):
        codes = [code_ref[target * 8 + d] for d in range(8)]
        row_out = 0
        row_in = 0
        for channels, length in specs:
            rows_in = channels * length // 32

            def frame(code):
                rows = gathered[code & 31, row_in : row_in + rows_in, :]
                if length == 64:
                    return jnp.concatenate([rows[:channels], rows[channels:]], axis=1)
                if length == 16:
                    low = lanes_of(128) < 64
                    wide = rows.astype(F32)
                    split = [jnp.where(low, wide, 0.0), jnp.where(low, 0.0, wide)]
                    return jnp.concatenate(split, axis=0).astype(BF16)
                return rows

            depth = 256 if length == 64 else 128
            source = lax.broadcasted_iota(jnp.int32, (depth, 128), 0)
            if length == 16:
                source = source & 63
            lane = lanes_of(128)
            for block in BLOCKS[length]:
                total = None
                for d, base in block:
                    code = codes[d]
                    edge = (code >> 5) & 3
                    flip = (code >> 7) & 1
                    active = (code >> 8) == wanted
                    start = edge * length + flip * (length - 1)
                    if d < 4:
                        target_cell = start + (1 - 2 * flip) * (lane - base)
                        inside = (lane >= base) & (lane < base + length)
                    else:
                        target_cell = start + jnp.zeros_like(lane)
                        inside = lane == base
                    target_cell = jnp.where(inside & active, target_cell, -1)
                    chosen = jnp.where(source == target_cell, 1.0, 0.0).astype(BF16)
                    piece = dot(frame(code), chosen)
                    total = piece if total is None else total + piece
                out[row_out : row_out + channels, :] = total.astype(BF16)
                row_out += channels
            row_in += rows_in


def pick(codes, gathered, specs):
    rows = sum(channels * len(BLOCKS[length]) for channels, length in specs)
    shape = jax.ShapeDtypeStruct((rows, 128), BF16)
    return pl.pallas_call(
        functools.partial(pick_kernel, specs=specs),
        out_shape=(shape, shape, shape),
        in_specs=[pl.BlockSpec(memory_space=pltpu.SMEM), pl.BlockSpec(memory_space=pltpu.VMEM)],
        name="pick",
    )(codes, gathered)


def call(kernel, shapes, *args, name):
    return pl.pallas_call(
        kernel,
        out_shape=tuple(jax.ShapeDtypeStruct(s, t) for s, t in shapes),
        name=name,
    )(*args)


def start_kernel(x_ref, film_ref, wet_ref, a_ref, frame_ref):
    a = activate(x_ref[...].astype(F32), film_of(film_ref, 1))
    a_ref[...] = a
    frame_ref[...] = frame_64(a, wet_ref[...])


def finish_1(base, x, own, down, up, w, we, cm, wet, c64, x32t, film, skip_ref, a_ref, frame_ref, skip_frame_ref):
    halo = halo_of(own, down, up, 0, 32, 3).astype(BF16)
    first = x[...].astype(F32) + with_halo_64(base[...], halo, w[...], we[...], cm[...])
    skip = first.astype(BF16)
    skip_ref[...] = skip
    a = activate(by_chunks(first, c64[...]), film_of(film, 2))
    a_ref[...] = a
    frame_ref[...] = dot(a, x32t[...]).astype(BF16)
    skip_frame_ref[...] = frame_64(skip, wet[...])


def finish_2(base, own, down, up, w, x32, c32, x32t, low_t, high_t, film, skip_ref, a_ref, frame_ref, skip_frame_ref):
    halo = halo_of(own, down, up, 0, 32, 2).astype(BF16)
    second = with_halo(base[...], halo, w[...], 32, x32[...])
    skip = second.astype(BF16)
    skip_ref[...] = skip
    a = activate(by_chunks(second, c32[...]), film_of(film, 3))
    a_ref[...] = a
    frame_ref[...] = frame_16(a, low_t[...], high_t[...])
    skip_frame_ref[...] = dot(skip, x32t[...]).astype(BF16)


def finish_3(base, own, down, up, w, x16, low_t, high_t, film, third_ref, a_ref, frame_ref):
    halo = halo_of(own, down, up, 0, 64, 1).astype(BF16)
    third = with_halo(base[...], halo, w[...], 16, x16[...])
    third_ref[...] = third
    a = activate(third, film_of(film, 4))
    a_ref[...] = a
    frame_ref[...] = frame_16(a, low_t[...], high_t[...])


def finish_4(base, third, own, down, up, w, x16, low_t, high_t, r32, skip, skip_frame, film, a_ref, frame_ref):
    halo = halo_of(own, down, up, 0, 128, 1).astype(BF16)
    fourth = third[...] + with_halo(base[...], halo, w[...], 16, x16[...])
    frame_ref[0:64, :] = frame_16(fourth.astype(BF16), low_t[...], high_t[...])
    frame_ref[64:128, :] = skip_frame[...]
    joined = jnp.concatenate([by_chunks(fourth, r32[...]), skip[...].astype(F32)], axis=0)
    a_ref[...] = activate(joined, film_of(film, 5))


def finish_5(base, own, down, up, w, x32, x32t, double, r64, skip, skip_frame, film, a_ref, frame_ref):
    coarse = dot(halo_of(own, down, up, 0, 128, 1).astype(BF16), double[...])
    halo = activate(jnp.concatenate([coarse, halo_of(own, down, up, 128, 64, 2)], axis=0), film_of(film, 5))
    fifth = with_halo(base[...], halo, w[...], 32, x32[...])
    frame_ref[0:64, :] = dot(fifth.astype(BF16), x32t[...]).astype(BF16)
    frame_ref[64:128, :] = skip_frame[...]
    joined = jnp.concatenate([by_chunks(fifth, r64[...]), skip[...].astype(F32)], axis=0)
    a_ref[...] = activate(joined, film_of(film, 6))


def finish_6(base, own, down, up, w, we, cm, double, skip, film, out_ref):
    coarse = dot(halo_of(own, down, up, 0, 64, 2).astype(BF16), double[...])
    halo = activate(jnp.concatenate([coarse, halo_of(own, down, up, 128, 32, 3)], axis=0), film_of(film, 6))
    total = with_halo_64(base[...], halo, w[...], we[...], cm[...])
    out_ref[...] = (skip[...].astype(F32) + total).astype(BF16)


def one_hot(targets, width):
    return (jnp.asarray(targets, jnp.int32)[:, None] == lax.broadcasted_iota(jnp.int32, (1, width), 1)).astype(BF16)


def border_targets(length, width):
    cells = length * length
    k = np.arange(length)
    targets = np.full(width, -1)
    edges = [k, cells - length + k, k * length, k * length + length - 1]
    targets[: 4 * length] = np.concatenate(edges)
    targets[4 * length : 4 * length + 4] = [0, length - 1, cells - length, cells - 1]
    return targets


def chunk_targets(length):
    lane = np.arange(512)
    return (lane // length // 2) * (length // 2) + (lane % length) // 2


def double_targets(length, width):
    targets = np.full(width, -1)
    lane = np.arange(4 * length)
    targets[: 4 * length] = (lane // length) * (length // 2) + (lane % length) // 2
    targets[4 * length : 4 * length + 4] = 2 * length + np.arange(4)
    return targets


def tap_rows(weight):
    out_channels = weight.shape[0]
    channels = weight.shape[1] // 9
    return weight.reshape(out_channels, 9, channels).transpose(1, 0, 2).reshape(9 * out_channels, channels)


def far_patch(patch):
    return (patch + 16) % 32


def face_moves(by):
    moves = []
    for face in range(8):
        jump = face % 4 == (3 if by == 1 else 0)
        for patch in range(32):
            moves.append((face * 32 + patch, (face + by) % 8 * 32 + (far_patch(patch) if jump else patch)))
    return moves


def link_codes(link_patch, link_shift, link_turn):
    edge_table = TURN_EDGE[:, READ_EDGE]
    flip_table = TURN_FLIP[:, READ_EDGE] ^ READ_END[None, :]
    packed = edge_table * 32 + flip_table * 128
    extra = jnp.full(link_turn.shape, 0, jnp.int32)
    for turn in range(4):
        extra = jnp.where(link_turn == turn, jnp.asarray(packed[turn], jnp.int32), extra)
    codes = link_patch + extra + (link_shift + 1) * 256
    face = lax.axis_index("face")
    patch = lax.axis_index("patch")
    up_patch = jnp.where(face % 4 == 3, far_patch(patch), patch)
    down_patch = jnp.where(face % 4 == 0, far_patch(patch), patch)
    flat = codes.reshape(256, 8)
    rows = [face * 32 + patch, (face + 1) % 8 * 32 + up_patch, (face + 7) % 8 * 32 + down_patch]
    return jnp.concatenate([lax.dynamic_slice(flat, (row, 0), (1, 8)) for row in rows], axis=0).reshape(24)


def body(
    features,
    film_first,
    weight_first,
    film_second,
    weight_second,
    film_third,
    weight_third,
    film_fourth,
    weight_fourth,
    film_fifth,
    weight_fifth,
    film_sixth,
    weight_sixth,
    link_patch,
    link_shift,
    link_turn,
):
    x = features[:, 0, :]
    film = jnp.concatenate([film_first, film_second, film_third, film_fourth, film_fifth, film_sixth], axis=1).T
    codes = link_codes(link_patch, link_shift, link_turn)
    w1, w2, w3, w4, w5, w6 = [
        tap_rows(w) for w in (weight_first, weight_second, weight_third, weight_fourth, weight_fifth, weight_sixth)
    ]
    k = np.arange(64)
    we = one_hot(np.concatenate([k * 64, k * 64 + 63]), 4096)
    wet = we.T
    cm = one_hot(np.concatenate([[0, 63, 64, 127], np.full(124, -1)]), 128)
    x32 = one_hot(border_targets(32, 256), 1024)
    x32t = one_hot(border_targets(32, 256)[:128], 1024).T
    x16 = one_hot(border_targets(16, 128), 256)
    edges16 = border_targets(16, 128)[:64]
    none16 = np.full(64, -1)
    low_t = one_hot(np.concatenate([edges16, none16]), 256).T
    high_t = one_hot(np.concatenate([none16, edges16]), 256).T
    r64 = one_hot(chunk_targets(64), 128).T
    r32 = one_hot(chunk_targets(32), 128).T
    c64 = one_hot(chunk_targets(64), 128) * jnp.asarray(0.25, BF16)
    c32 = one_hot(chunk_targets(32), 128) * jnp.asarray(0.25, BF16)
    double32 = one_hot(double_targets(32, 256), 128).T
    double64 = one_hot(double_targets(64, 384), 256).T
    above = face_moves(1)
    below = face_moves(-1)

    def exchange(frame, specs):
        copies = jnp.broadcast_to(frame[None], (32, *frame.shape))
        gathered = lax.all_to_all(copies, "patch", split_axis=0, concat_axis=0, tiled=True)
        own, for_up, for_down = pick(codes, gathered, specs)
        from_down = lax.ppermute(for_up, ("face", "patch"), above)
        from_up = lax.ppermute(for_down, ("face", "patch"), below)
        return own, from_down, from_up

    a1, f1 = call(start_kernel, [((32, 4096), BF16), ((64, 128), BF16)], x, film, wet, name="start")
    h = exchange(f1, ((32, 64),))
    base = main_conv(a1, w1, 64)
    skip_fine, a2, f2, fine_frame = call(
        finish_1,
        [((32, 4096), BF16), ((32, 1024), BF16), ((32, 128), BF16), ((64, 128), BF16)],
        base, x, *h, w1, we, cm, wet, c64, x32t, film,
        name="finish_1",
    )
    h = exchange(f2, ((32, 32),))
    base = main_conv(a2, w2, 32)
    skip_middle, a3, f3, middle_frame = call(
        finish_2,
        [((64, 1024), BF16), ((64, 256), BF16), ((32, 128), BF16), ((64, 128), BF16)],
        base, *h, w2, x32, c32, x32t, low_t, high_t, film,
        name="finish_2",
    )
    h = exchange(f3, ((64, 16),))
    base = main_conv(a3, w3, 16)
    third, a4, f4 = call(
        finish_3,
        [((128, 256), F32), ((128, 256), BF16), ((64, 128), BF16)],
        base, *h, w3, x16, low_t, high_t, film,
        name="finish_3",
    )
    h = exchange(f4, ((128, 16),))
    base = main_conv(a4, w4, 16)
    a5, f5 = call(
        finish_4,
        [((192, 1024), BF16), ((128, 128), BF16)],
        base, third, *h, w4, x16, low_t, high_t, r32, skip_middle, middle_frame, film,
        name="finish_4",
    )
    h = exchange(f5, ((128, 16), (64, 32)))
    base = main_conv(a5, w5, 32)
    a6, f6 = call(
        finish_5,
        [((96, 4096), BF16), ((128, 128), BF16)],
        base, *h, w5, x32, x32t, double32, r64, skip_fine, fine_frame, film,
        name="finish_5",
    )
    h = exchange(f6, ((64, 32), (32, 64)))
    base = main_conv(a6, w6, 64)
    (result,) = call(
        finish_6,
        [((32, 4096), BF16)],
        base, *h, w6, we, cm, double64, skip_fine, film,
        name="finish_6",
    )
    return result[:, None, :]


def solution(mesh):
    in_specs = (P(None, "face", "patch"),) + (P(),) * 15
    out_specs = P(None, "face", "patch")
    return jax.shard_map(body, mesh=mesh, in_specs=in_specs, out_specs=out_specs, check_vma=False)
```

```python
import functools

import jax
import jax.numpy as jnp
import numpy as np
from jax import lax
from jax.experimental import pallas as pl
from jax.experimental.pallas import tpu as pltpu
from jax.sharding import PartitionSpec as P

EPSILON = 1e-05
FLOOR_SQUARE = 0.5
F32 = jnp.float32
BF16 = jnp.bfloat16
LIMIT = pltpu.CompilerParams(vmem_limit_bytes=24 * 1024 * 1024)
FILM_ROWS = {1: (0, 32), 2: (32, 64), 3: (64, 128), 4: (128, 256), 5: (256, 448), 6: (448, 544)}
TURN_EDGE = np.array([[0, 1, 2, 3], [3, 2, 0, 1], [1, 0, 3, 2], [2, 3, 1, 0]])
TURN_FLIP = np.array([[0, 0, 0, 0], [0, 0, 1, 1], [1, 1, 1, 1], [1, 1, 0, 0]])
READ_EDGE = np.array([1, 0, 3, 2, 1, 1, 0, 0])
READ_END = np.array([0, 0, 0, 0, 1, 0, 1, 0])
CORNERS = [(4, 0), (5, 1), (6, 2), (7, 3)]
BLOCKS = {
    64: [[(0, 0), (1, 64)], [(2, 0), (3, 64)], CORNERS],
    32: [[(0, 0), (1, 32), (2, 64), (3, 96)], CORNERS],
    16: [[(0, 0), (1, 16), (2, 32), (3, 48), (4, 64), (5, 65), (6, 66), (7, 67)]],
}


def dot(a, b):
    return jnp.dot(a, b, preferred_element_type=F32)


def in_vmem(x):
    return pltpu.with_memory_space_constraint(x, pltpu.VMEM)


def lanes_of(width):
    return lax.broadcasted_iota(jnp.int32, (1, width), 1)


def halves(x):
    high = x.astype(BF16)
    return high, (x - high.astype(F32)).astype(BF16)


def activate(values, film):
    mean_square = jnp.mean(values * values, axis=0, keepdims=True)
    if values.shape[0] >= 64:
        inverse = lax.rsqrt(mean_square + EPSILON)
    else:
        inverse = lax.rsqrt(jnp.maximum(mean_square, FLOOR_SQUARE))
    shaped = values * inverse * (1.0 + film[:, 0:1]) + film[:, 1:2]
    return (shaped / (1.0 + jnp.exp(-shaped))).astype(BF16)


def film_of(ref, index):
    first, last = FILM_ROWS[index]
    return ref[first:last, :]


def by_chunks(x, matrix):
    channels = x.shape[0]
    run = matrix.shape[0]
    count = x.shape[1] // run
    stacked = jnp.concatenate([x[:, run * k : run * (k + 1)] for k in range(count)], axis=0)
    high, low = halves(stacked)
    result = dot(high, matrix) + dot(low, matrix)
    return jnp.concatenate([result[channels * k : channels * (k + 1)] for k in range(count)], axis=1)


def frame_64(a, west_east_t):
    cells = a.shape[1]
    upper = jnp.where(lanes_of(128) < 64, a[:, :128].astype(F32), a[:, cells - 128 :].astype(F32))
    return jnp.concatenate([upper, dot(a, west_east_t)], axis=1).astype(BF16)


def put_slots(stage, first, frame, length):
    groups = 64 // length
    rows = frame.shape[0] // groups
    patch = lax.axis_index("patch")
    row, column = patch // 8, patch % 8
    outer = jnp.where(row == 0, 0, jnp.where(row == 3, 1, jnp.where(column == 0, 2, 3)))
    source = lax.broadcasted_iota(jnp.int32, (frame.shape[1], 128), 0)

    def placed(edge, half):
        total = None
        for group in range(groups):
            place = lanes_of(128) - (2 * group + half) * length
            wanted = jnp.where((place >= 0) & (place < length), edge * length + place, -1)
            chosen = jnp.where(source == wanted, 1.0, 0.0).astype(BF16)
            piece = dot(frame[group * rows : (group + 1) * rows], chosen)
            total = piece if total is None else total + piece
        return total

    shared = placed(outer, 0)
    for edge in range(4):
        stage[edge, first : first + rows, :] = (shared + placed(edge, 1)).astype(BF16)


def send_slots(stage, out):
    patch = lax.axis_index("patch")
    row, column = patch // 8, patch % 8
    second = jnp.where(column == 0, 2, 3)
    for target in range(32):
        down = target // 8 - row
        right = target % 8 - column
        near = (down >= -1) & (down <= 1) & (right >= -1) & (right <= 1) & (target != patch)
        across = jnp.where(right > 0, 3, 2)
        inner = jnp.where(down > 0, 1, jnp.where(down < 0, 0, across))
        out[target] = stage[jnp.where(near, inner, second)]


def halo_of(own, down, up, first, channels, blocks):
    rows = slice(first, first + channels * blocks)
    packed = own[rows, :].astype(F32) + down[rows, :].astype(F32) + up[rows, :].astype(F32)
    return jnp.concatenate([packed[channels * k : channels * (k + 1)] for k in range(blocks)], axis=1)


def expand(z, matrix):
    high, low = halves(z)
    both = dot(jnp.concatenate([high, low], axis=0), matrix)
    return both[: z.shape[0]] + both[z.shape[0] :]


def border_sums(halo, weight, length):
    products = dot(weight, halo)
    out_channels = weight.shape[0] // 9
    width = halo.shape[1]

    def tap(u, v):
        t = 3 * (u + 1) + v + 1
        return products[t * out_channels : (t + 1) * out_channels]

    lane = lanes_of(width)
    part = lane // length
    place = lane % length

    def along(step):
        return jnp.where(
            part == 0,
            tap(-1, step),
            jnp.where(part == 1, tap(1, step), jnp.where(part == 2, tap(step, -1), tap(step, 1))),
        )

    end = 4 * length
    corner = jnp.where(lane == end, tap(-1, -1), 0.0)
    corner = jnp.where(lane == end + 1, tap(-1, 1), corner)
    corner = jnp.where(lane == end + 2, tap(1, -1), corner)
    corner = jnp.where(lane == end + 3, tap(1, 1), corner)
    edge = part < 4
    before = jnp.where(edge & (place != 0), pltpu.roll(along(-1), 1, 1), 0.0)
    after = jnp.where(edge & (place != length - 1), pltpu.roll(along(1), width - 1, 1), 0.0)
    return jnp.where(edge, along(0), corner) + before + after


def with_halo_64(base, halo, weight, west_east, corner_map):
    sums = border_sums(halo, weight, 64)
    rows = sums[:, :128] + expand(sums[:, 256:], corner_map)
    total = base + expand(sums[:, 128:256], west_east)
    cells = total.shape[1]
    low = lanes_of(128) < 64
    top = total[:, :128] + jnp.where(low, rows, 0.0)
    bottom = total[:, cells - 128 :] + jnp.where(low, 0.0, rows)
    return jnp.concatenate([top, total[:, 128 : cells - 128], bottom], axis=1)


def with_halo(base, halo, weight, length, matrix):
    return base + expand(border_sums(halo, weight, length), matrix)


def main_kernel(a_ref, w_ref, out_ref, products, *, length):
    products[...] = dot(w_ref[...], a_ref[...])
    out_channels, cells = out_ref.shape
    lane = lanes_of(cells)
    place = lane % length

    def tap(u, v):
        t = 3 * (u + 1) + v + 1
        return products[t * out_channels : (t + 1) * out_channels, :]

    def column(v):
        above = jnp.where(lane < length, 0.0, pltpu.roll(tap(-1, v), length, 1))
        below = jnp.where(lane >= cells - length, 0.0, pltpu.roll(tap(1, v), cells - length, 1))
        return tap(0, v) + above + below

    total = column(0)
    total += jnp.where(place == 0, 0.0, pltpu.roll(column(-1), 1, 1))
    total += jnp.where(place == length - 1, 0.0, pltpu.roll(column(1), cells - 1, 1))
    out_ref[...] = total


def main_conv(a, weight, length):
    taps_out = weight.shape[0]
    cells = a.shape[1]
    return pl.pallas_call(
        functools.partial(main_kernel, length=length),
        out_shape=jax.ShapeDtypeStruct((taps_out // 9, cells), F32),
        scratch_shapes=[pltpu.VMEM((taps_out, cells), F32)],
        cost_estimate=pl.CostEstimate(
            flops=2 * taps_out * weight.shape[1] * cells * 8, bytes_accessed=a.size * 2 + taps_out * cells, transcendentals=0
        ),
        compiler_params=LIMIT,
        name="main_conv",
    )(in_vmem(a), in_vmem(weight))


def pick_kernel(code_ref, gathered, *outs, specs):
    for target, out in enumerate(outs):
        codes = [code_ref[target * 8 + d] for d in range(8)]
        row_out = 0
        row_in = 0
        for channels, length in specs:
            groups = 64 // length
            rows_in = channels // groups
            lane = lanes_of(128)
            source = lax.broadcasted_iota(jnp.int32, (128, 128), 0) & (2 * length - 1)

            def frame(code):
                rows = gathered[code & 31, row_in : row_in + rows_in, :]
                if groups == 1:
                    return rows
                wide = rows.astype(F32)
                split = [jnp.where(lane // (2 * length) == group, wide, 0.0) for group in range(groups)]
                return jnp.concatenate(split, axis=0).astype(BF16)

            for block in BLOCKS[length]:
                total = None
                for d, base in block:
                    code = codes[d]
                    half = (code >> 5) & 1
                    flip = (code >> 6) & 1
                    active = (code >> 7) == 1
                    start = half * length + flip * (length - 1)
                    if d < 4:
                        cell = start + (1 - 2 * flip) * (lane - base)
                        inside = (lane >= base) & (lane < base + length)
                    else:
                        cell = start + jnp.zeros_like(lane)
                        inside = lane == base
                    cell = jnp.where(inside & active, cell, -1)
                    chosen = jnp.where(source == cell, 1.0, 0.0).astype(BF16)
                    piece = dot(frame(code), chosen)
                    total = piece if total is None else total + piece
                out[row_out : row_out + channels, :] = total.astype(BF16)
                row_out += channels
            row_in += rows_in


def pick(codes, gathered, specs, targets):
    rows = sum(channels * len(BLOCKS[length]) for channels, length in specs)
    shape = jax.ShapeDtypeStruct((rows, 128), BF16)
    return pl.pallas_call(
        functools.partial(pick_kernel, specs=specs),
        out_shape=(shape,) * targets,
        in_specs=[pl.BlockSpec(memory_space=pltpu.SMEM), pl.BlockSpec(memory_space=pltpu.VMEM)],
        compiler_params=LIMIT,
        name="pick",
    )(codes, gathered)


def call(kernel, shapes, *args, stage=0):
    return pl.pallas_call(
        kernel,
        out_shape=tuple(jax.ShapeDtypeStruct(s, t) for s, t in shapes),
        scratch_shapes=[pltpu.VMEM((4, stage, 128), BF16)] if stage else [],
        compiler_params=LIMIT,
    )(*[in_vmem(x) for x in args])


def start_kernel(x_ref, film_ref, a_ref, slots, stage):
    square = [lax.broadcasted_iota(jnp.int32, (32, 32), dim) for dim in (0, 1)]
    columns = [
        jnp.sum(jnp.where(square[0] == square[1], film_ref[k : k + 1, :], 0.0), axis=1, keepdims=True) for k in (0, 1)
    ]
    a = activate(x_ref[...].astype(F32), jnp.concatenate(columns, axis=1))
    a_ref[...] = a
    cell = lax.broadcasted_iota(jnp.int32, (4096, 128), 0)
    lane = lanes_of(128)
    wanted = jnp.where(lane < 64, lane * 64, (lane - 64) * 64 + 63)
    put_slots(stage, 0, frame_64(a, jnp.where(cell == wanted, 1.0, 0.0).astype(BF16)), 64)
    send_slots(stage, slots)


def finish_1(base, x, own, down, up, w, we, cm, wet, c64, x32t, film, skip_ref, a_ref, slots, skip_frame_ref, stage):
    halo = halo_of(own, down, up, 0, 32, 3).astype(BF16)
    first = x[...].astype(F32) + with_halo_64(base[...], halo, w[...], we[...], cm[...])
    skip = first.astype(BF16)
    skip_ref[...] = skip
    a = activate(by_chunks(first, c64[...]), film_of(film, 2))
    a_ref[...] = a
    put_slots(stage, 0, dot(a, x32t[...]).astype(BF16), 32)
    send_slots(stage, slots)
    skip_frame_ref[...] = frame_64(skip, wet[...])


def finish_2(base, own, down, up, w, x32, c32, x32t, x16t, film, skip_ref, a_ref, slots, skip_frame_ref, stage):
    halo = halo_of(own, down, up, 0, 32, 2).astype(BF16)
    second = with_halo(base[...], halo, w[...], 32, x32[...])
    skip = second.astype(BF16)
    skip_ref[...] = skip
    a = activate(by_chunks(second, c32[...]), film_of(film, 3))
    a_ref[...] = a
    put_slots(stage, 0, dot(a, x16t[...]).astype(BF16), 16)
    send_slots(stage, slots)
    skip_frame_ref[...] = dot(skip, x32t[...]).astype(BF16)


def finish_3(base, own, down, up, w, x16, x16t, film, third_ref, a_ref, slots, stage):
    halo = halo_of(own, down, up, 0, 64, 1).astype(BF16)
    third = with_halo(base[...], halo, w[...], 16, x16[...])
    third_ref[...] = third
    a = activate(third, film_of(film, 4))
    a_ref[...] = a
    put_slots(stage, 0, dot(a, x16t[...]).astype(BF16), 16)
    send_slots(stage, slots)


def finish_4(base, third, own, down, up, w, x16, x16t, r32, skip, skip_frame, film, a_ref, slots, stage):
    halo = halo_of(own, down, up, 0, 128, 1).astype(BF16)
    fourth = third[...] + with_halo(base[...], halo, w[...], 16, x16[...])
    put_slots(stage, 0, dot(fourth.astype(BF16), x16t[...]).astype(BF16), 16)
    put_slots(stage, 32, skip_frame[...], 32)
    send_slots(stage, slots)
    joined = jnp.concatenate([by_chunks(fourth, r32[...]), skip[...].astype(F32)], axis=0)
    a_ref[...] = activate(joined, film_of(film, 5))


def finish_5(base, own, down, up, w, x32, x32t, double, r64, skip, skip_frame, film, a_ref, slots, stage):
    coarse = dot(halo_of(own, down, up, 0, 128, 1).astype(BF16), double[...])
    halo = activate(jnp.concatenate([coarse, halo_of(own, down, up, 128, 64, 2)], axis=0), film_of(film, 5))
    fifth = with_halo(base[...], halo, w[...], 32, x32[...])
    put_slots(stage, 0, dot(fifth.astype(BF16), x32t[...]).astype(BF16), 32)
    put_slots(stage, 32, skip_frame[...], 64)
    send_slots(stage, slots)
    joined = jnp.concatenate([by_chunks(fifth, r64[...]), skip[...].astype(F32)], axis=0)
    a_ref[...] = activate(joined, film_of(film, 6))


def finish_6(base, own, down, up, w, we, cm, double, skip, film, out_ref):
    coarse = dot(halo_of(own, down, up, 0, 64, 2).astype(BF16), double[...])
    halo = activate(jnp.concatenate([coarse, halo_of(own, down, up, 128, 32, 3)], axis=0), film_of(film, 6))
    total = with_halo_64(base[...], halo, w[...], we[...], cm[...])
    out_ref[...] = (skip[...].astype(F32) + total).astype(BF16)


def one_hot(targets, width):
    return (jnp.asarray(targets, jnp.int32)[:, None] == lax.broadcasted_iota(jnp.int32, (1, width), 1)).astype(BF16)


def border_targets(length, width):
    cells = length * length
    k = np.arange(length)
    targets = np.full(width, -1)
    edges = [k, cells - length + k, k * length, k * length + length - 1]
    targets[: 4 * length] = np.concatenate(edges)
    targets[4 * length : 4 * length + 4] = [0, length - 1, cells - length, cells - 1]
    return targets


def chunk_targets(length):
    lane = np.arange(512)
    return (lane // length // 2) * (length // 2) + (lane % length) // 2


def double_targets(length, width):
    targets = np.full(width, -1)
    lane = np.arange(4 * length)
    targets[: 4 * length] = (lane // length) * (length // 2) + (lane % length) // 2
    targets[4 * length : 4 * length + 4] = 2 * length + np.arange(4)
    return targets


def tap_rows(weight):
    out_channels = weight.shape[0]
    channels = weight.shape[1] // 9
    return weight.reshape(out_channels, 9, channels).transpose(1, 0, 2).reshape(9 * out_channels, channels)


NEAR_RELAY = {p: p for p in (0, 3, 4, 7, 24, 27, 28, 31)}
NEAR_RELAY |= {1: 2, 2: 10, 8: 11, 6: 5, 5: 13, 15: 12, 25: 26, 26: 18, 16: 19, 30: 29, 29: 21, 23: 20}
FAR_RELAY = {0: 26, 1: 27, 2: 18, 3: 19, 8: 24, 16: 0, 24: 2, 25: 3, 26: 10, 27: 11}
FAR_RELAY |= {7: 29, 6: 28, 5: 21, 4: 20, 15: 31, 23: 7, 31: 5, 30: 4, 29: 13, 28: 12}


def other_face(face, kind):
    return face ^ 1 if kind == 0 else (face + 1 if face % 2 else face - 1) % 8


def face_moves(kind):
    moves = []
    for face in range(8):
        far = kind == 1 and face % 4 in (0, 3)
        for target, relay in (FAR_RELAY if far else NEAR_RELAY).items():
            moves.append((face * 32 + relay, other_face(face, kind) * 32 + target))
    return moves


def inverse(relays):
    targets = np.full(32, -1)
    for target, relay in relays.items():
        targets[relay] = target
    return targets


def link_codes(link_patch, link_shift, link_turn):
    packed = TURN_EDGE[:, READ_EDGE] * 2 + (TURN_FLIP[:, READ_EDGE] ^ READ_END[None, :])
    choice = jnp.zeros(link_turn.shape, jnp.int32)
    for turn in range(4):
        choice = jnp.where(link_turn == turn, jnp.asarray(packed[turn], jnp.int32), choice)
    edge, flip = choice // 2, choice % 2
    row, column = link_patch // 8, link_patch % 8
    outer = jnp.where(row == 0, 0, jnp.where(row == 3, 1, jnp.where(column == 0, 2, 3)))
    cell_row = jnp.where(edge < 2, edge, flip)
    cell_column = jnp.where(edge < 2, flip, edge - 2)
    in_first = jnp.where(outer < 2, cell_row == outer, cell_column == outer - 2)
    is_corner = jnp.asarray(np.arange(8) >= 4)
    half = jnp.where(is_corner, jnp.where(in_first, 0, 1), jnp.where(edge == outer, 0, 1))
    corner_flip = jnp.where(in_first & (outer < 2), cell_column, cell_row)
    inside = link_shift == 0
    half = jnp.where(inside, 1, half)
    flip = jnp.where(is_corner, jnp.where(inside, cell_column, corner_flip), flip)
    flat = (link_patch + half * 32 + flip * 64 + (link_shift + 1) * 128).reshape(256, 8)
    face = lax.axis_index("face")
    patch = lax.axis_index("patch")
    odd = face % 2
    this = np.arange(32) == patch
    near = jnp.sum(jnp.where(this, jnp.asarray(inverse(NEAR_RELAY), jnp.int32), 0))
    far = jnp.sum(jnp.where(this, jnp.asarray(inverse(FAR_RELAY), jnp.int32), 0))
    far = jnp.where((face % 4 == 0) | (face % 4 == 3), far, near)
    places = [
        (face, patch, 1),
        (face + 1 - 2 * odd, near, 2 * odd),
        ((face + 7 + 2 * odd) % 8, far, 2 - 2 * odd),
    ]
    rows = []
    for of_face, of_patch, shift in places:
        chosen = lax.dynamic_slice(flat, (of_face * 32 + jnp.maximum(of_patch, 0), 0), (1, 8))
        active = (chosen // 128 == shift) & (of_patch >= 0)
        rows.append(chosen % 128 + jnp.where(active, 128, 0))
    return jnp.concatenate(rows, axis=0).reshape(24)


def body(
    features,
    film_first,
    weight_first,
    film_second,
    weight_second,
    film_third,
    weight_third,
    film_fourth,
    weight_fourth,
    film_fifth,
    weight_fifth,
    film_sixth,
    weight_sixth,
    link_patch,
    link_shift,
    link_turn,
):
    x = features[:, 0, :]
    film = jnp.concatenate([film_first, film_second, film_third, film_fourth, film_fifth, film_sixth], axis=1).T
    codes = link_codes(link_patch, link_shift, link_turn)
    w1, w2, w3, w4, w5, w6 = [
        tap_rows(w) for w in (weight_first, weight_second, weight_third, weight_fourth, weight_fifth, weight_sixth)
    ]
    k = np.arange(64)
    we = one_hot(np.concatenate([k * 64, k * 64 + 63]), 4096)
    wet = we.T
    cm = one_hot(np.concatenate([[0, 63, 64, 127], np.full(124, -1)]), 128)
    x32 = one_hot(border_targets(32, 256), 1024)
    x32t = one_hot(border_targets(32, 256)[:128], 1024).T
    x16 = one_hot(border_targets(16, 128), 256)
    x16t = one_hot(np.where(np.arange(128) < 64, border_targets(16, 128), -1), 256).T
    r64 = one_hot(chunk_targets(64), 128).T
    r32 = one_hot(chunk_targets(32), 128).T
    c64 = one_hot(chunk_targets(64), 128) * jnp.asarray(0.25, BF16)
    c32 = one_hot(chunk_targets(32), 128) * jnp.asarray(0.25, BF16)
    double32 = one_hot(double_targets(32, 256), 128).T
    double64 = one_hot(double_targets(64, 384), 256).T
    near_moves = face_moves(0)
    far_moves = face_moves(1)

    def exchange(slots, specs):
        gathered = lax.all_to_all(slots, "patch", split_axis=0, concat_axis=0, tiled=True)
        gathered = in_vmem(gathered)
        for_near, for_far = pick(codes[8:], gathered, specs, 2)
        from_far = lax.ppermute(for_far, ("face", "patch"), far_moves)
        from_near = lax.ppermute(for_near, ("face", "patch"), near_moves)
        (own,) = pick(codes[:8], gathered, specs, 1)
        return own, from_near, from_far

    a1, f1 = call(start_kernel, [((32, 4096), BF16), ((32, 32, 128), BF16)], x, film_first, stage=32)
    h = exchange(f1, ((32, 64),))
    base = main_conv(a1, w1, 64)
    skip_fine, a2, f2, fine_frame = call(
        finish_1,
        [((32, 4096), BF16), ((32, 1024), BF16), ((32, 16, 128), BF16), ((32, 256), BF16)],
        base, x, *h, w1, we, cm, wet, c64, x32t, film,
        stage=16,
    )
    h = exchange(f2, ((32, 32),))
    base = main_conv(a2, w2, 32)
    skip_middle, a3, f3, middle_frame = call(
        finish_2,
        [((64, 1024), BF16), ((64, 256), BF16), ((32, 16, 128), BF16), ((64, 128), BF16)],
        base, *h, w2, x32, c32, x32t, x16t, film,
        stage=16,
    )
    h = exchange(f3, ((64, 16),))
    base = main_conv(a3, w3, 16)
    third, a4, f4 = call(
        finish_3,
        [((128, 256), F32), ((128, 256), BF16), ((32, 32, 128), BF16)],
        base, *h, w3, x16, x16t, film,
        stage=32,
    )
    h = exchange(f4, ((128, 16),))
    base = main_conv(a4, w4, 16)
    a5, f5 = call(
        finish_4,
        [((192, 1024), BF16), ((32, 64, 128), BF16)],
        base, third, *h, w4, x16, x16t, r32, skip_middle, middle_frame, film,
        stage=64,
    )
    h = exchange(f5, ((128, 16), (64, 32)))
    base = main_conv(a5, w5, 32)
    a6, f6 = call(
        finish_5,
        [((96, 4096), BF16), ((32, 64, 128), BF16)],
        base, *h, w5, x32, x32t, double32, r64, skip_fine, fine_frame, film,
        stage=64,
    )
    h = exchange(f6, ((64, 32), (32, 64)))
    base = main_conv(a6, w6, 64)
    (result,) = call(
        finish_6,
        [((32, 4096), BF16)],
        base, *h, w6, we, cm, double64, skip_fine, film,
    )
    return result[:, None, :]


def solution(mesh):
    in_specs = (P(None, "face", "patch"),) + (P(),) * 15
    out_specs = P(None, "face", "patch")
    return jax.shard_map(body, mesh=mesh, in_specs=in_specs, out_specs=out_specs, check_vma=False)
```

```python
import functools

import jax
import jax.numpy as jnp
import numpy as np
from jax import lax
from jax.experimental import pallas as pl
from jax.experimental.pallas import tpu as pltpu
from jax.sharding import PartitionSpec as P

EPSILON = 1e-05
FLOOR_SQUARE = 0.5
F32 = jnp.float32
BF16 = jnp.bfloat16
LIMIT = pltpu.CompilerParams(vmem_limit_bytes=24 * 1024 * 1024)
FILM_ROWS = {1: (0, 32), 2: (32, 64), 3: (64, 128), 4: (128, 256), 5: (256, 448), 6: (448, 544)}
TURN_EDGE = np.array([[0, 1, 2, 3], [3, 2, 0, 1], [1, 0, 3, 2], [2, 3, 1, 0]])
TURN_FLIP = np.array([[0, 0, 0, 0], [0, 0, 1, 1], [1, 1, 1, 1], [1, 1, 0, 0]])
READ_EDGE = np.array([1, 0, 3, 2, 1, 1, 0, 0])
READ_END = np.array([0, 0, 0, 0, 1, 0, 1, 0])
CORNERS = [(4, 0), (5, 1), (6, 2), (7, 3)]
BLOCKS = {
    64: [[(0, 0), (1, 64)], [(2, 0), (3, 64)], CORNERS],
    32: [[(0, 0), (1, 32), (2, 64), (3, 96)], CORNERS],
    16: [[(0, 0), (1, 16), (2, 32), (3, 48), (4, 64), (5, 65), (6, 66), (7, 67)]],
}


def dot(a, b):
    return jnp.dot(a, b, preferred_element_type=F32)


def in_vmem(x):
    return pltpu.with_memory_space_constraint(x, pltpu.VMEM)


def lanes_of(width):
    return lax.broadcasted_iota(jnp.int32, (1, width), 1)


def halves(x):
    high = x.astype(BF16)
    return high, (x - high.astype(F32)).astype(BF16)


def activate(values, film):
    mean_square = jnp.mean(values * values, axis=0, keepdims=True)
    if values.shape[0] >= 64:
        inverse = lax.rsqrt(mean_square + EPSILON)
    else:
        inverse = lax.rsqrt(jnp.maximum(mean_square, FLOOR_SQUARE))
    shaped = values * inverse * (1.0 + film[:, 0:1]) + film[:, 1:2]
    return (shaped / (1.0 + jnp.exp(-shaped))).astype(BF16)


def film_of(ref, index):
    first, last = FILM_ROWS[index]
    return ref[first:last, :]


def by_chunks(x, matrix):
    channels = x.shape[0]
    run = matrix.shape[0]
    count = x.shape[1] // run
    stacked = jnp.concatenate([x[:, run * k : run * (k + 1)] for k in range(count)], axis=0)
    high, low = halves(stacked)
    result = dot(high, matrix) + dot(low, matrix)
    return jnp.concatenate([result[channels * k : channels * (k + 1)] for k in range(count)], axis=1)


def frame_64(a, west_east_t):
    cells = a.shape[1]
    upper = jnp.where(lanes_of(128) < 64, a[:, :128].astype(F32), a[:, cells - 128 :].astype(F32))
    return jnp.concatenate([upper, dot(a, west_east_t)], axis=1).astype(BF16)


def put_slots(stage, first, frame, length):
    groups = 64 // length
    rows = frame.shape[0] // groups
    patch = lax.axis_index("patch")
    row, column = patch // 8, patch % 8
    outer = jnp.where(row == 0, 0, jnp.where(row == 3, 1, jnp.where(column == 0, 2, 3)))
    source = lax.broadcasted_iota(jnp.int32, (frame.shape[1], 128), 0)

    def placed(edge, half):
        total = None
        for group in range(groups):
            place = lanes_of(128) - (2 * group + half) * length
            wanted = jnp.where((place >= 0) & (place < length), edge * length + place, -1)
            chosen = jnp.where(source == wanted, 1.0, 0.0).astype(BF16)
            piece = dot(frame[group * rows : (group + 1) * rows], chosen)
            total = piece if total is None else total + piece
        return total

    shared = placed(outer, 0)
    for edge in range(4):
        stage[edge, first : first + rows, :] = (shared + placed(edge, 1)).astype(BF16)


def send_slots(stage, out):
    patch = lax.axis_index("patch")
    row, column = patch // 8, patch % 8
    second = jnp.where(column == 0, 2, 3)
    for target in range(32):
        down = target // 8 - row
        right = target % 8 - column
        near = (down >= -1) & (down <= 1) & (right >= -1) & (right <= 1) & (target != patch)
        across = jnp.where(right > 0, 3, 2)
        inner = jnp.where(down > 0, 1, jnp.where(down < 0, 0, across))
        out[target] = stage[jnp.where(near, inner, second)]


def halo_of(own, down, up, first, channels, blocks):
    rows = slice(first, first + channels * blocks)
    packed = own[rows, :].astype(F32) + down[rows, :].astype(F32) + up[rows, :].astype(F32)
    return jnp.concatenate([packed[channels * k : channels * (k + 1)] for k in range(blocks)], axis=1)


def expand(z, matrix):
    high, low = halves(z)
    both = dot(jnp.concatenate([high, low], axis=0), matrix)
    return both[: z.shape[0]] + both[z.shape[0] :]


def border_sums(halo, weight, length):
    products = dot(weight, halo)
    out_channels = weight.shape[0] // 9
    width = halo.shape[1]

    def tap(u, v):
        t = 3 * (u + 1) + v + 1
        return products[t * out_channels : (t + 1) * out_channels]

    lane = lanes_of(width)
    part = lane // length
    place = lane % length

    def along(step):
        return jnp.where(
            part == 0,
            tap(-1, step),
            jnp.where(part == 1, tap(1, step), jnp.where(part == 2, tap(step, -1), tap(step, 1))),
        )

    end = 4 * length
    corner = jnp.where(lane == end, tap(-1, -1), 0.0)
    corner = jnp.where(lane == end + 1, tap(-1, 1), corner)
    corner = jnp.where(lane == end + 2, tap(1, -1), corner)
    corner = jnp.where(lane == end + 3, tap(1, 1), corner)
    edge = part < 4
    before = jnp.where(edge & (place != 0), pltpu.roll(along(-1), 1, 1), 0.0)
    after = jnp.where(edge & (place != length - 1), pltpu.roll(along(1), width - 1, 1), 0.0)
    return jnp.where(edge, along(0), corner) + before + after


def with_halo_64(base, halo, weight, west_east, corner_map):
    sums = border_sums(halo, weight, 64)
    rows = sums[:, :128] + expand(sums[:, 256:], corner_map)
    total = base + expand(sums[:, 128:256], west_east)
    cells = total.shape[1]
    low = lanes_of(128) < 64
    top = total[:, :128] + jnp.where(low, rows, 0.0)
    bottom = total[:, cells - 128 :] + jnp.where(low, 0.0, rows)
    return jnp.concatenate([top, total[:, 128 : cells - 128], bottom], axis=1)


def with_halo(base, halo, weight, length, matrix):
    return base + expand(border_sums(halo, weight, length), matrix)


def main_kernel(a_ref, w_ref, out_ref, products, *, length):
    products[...] = dot(w_ref[...], a_ref[...])
    out_channels, cells = out_ref.shape
    lane = lanes_of(cells)
    place = lane % length

    def tap(u, v):
        t = 3 * (u + 1) + v + 1
        return products[t * out_channels : (t + 1) * out_channels, :]

    def column(v):
        above = jnp.where(lane < length, 0.0, pltpu.roll(tap(-1, v), length, 1))
        below = jnp.where(lane >= cells - length, 0.0, pltpu.roll(tap(1, v), cells - length, 1))
        return tap(0, v) + above + below

    total = column(0)
    total += jnp.where(place == 0, 0.0, pltpu.roll(column(-1), 1, 1))
    total += jnp.where(place == length - 1, 0.0, pltpu.roll(column(1), cells - 1, 1))
    out_ref[...] = total


def main_conv(a, weight, length):
    taps_out = weight.shape[0]
    cells = a.shape[1]
    return pl.pallas_call(
        functools.partial(main_kernel, length=length),
        out_shape=jax.ShapeDtypeStruct((taps_out // 9, cells), F32),
        scratch_shapes=[pltpu.VMEM((taps_out, cells), F32)],
        cost_estimate=pl.CostEstimate(
            flops=2 * taps_out * weight.shape[1] * cells * 8, bytes_accessed=a.size * 2 + taps_out * cells, transcendentals=0
        ),
        compiler_params=LIMIT,
        name="main_conv",
    )(in_vmem(a), in_vmem(weight))


def pick_kernel(code_ref, gathered, *outs, specs):
    for target, out in enumerate(outs):
        codes = [code_ref[target * 8 + d] for d in range(8)]
        row_out = 0
        row_in = 0
        for channels, length in specs:
            groups = 64 // length
            rows_in = channels // groups
            lane = lanes_of(128)
            source = lax.broadcasted_iota(jnp.int32, (128, 128), 0) & (2 * length - 1)

            def frame(code):
                rows = gathered[code & 31, row_in : row_in + rows_in, :]
                if groups == 1:
                    return rows
                wide = rows.astype(F32)
                split = [jnp.where(lane // (2 * length) == group, wide, 0.0) for group in range(groups)]
                return jnp.concatenate(split, axis=0).astype(BF16)

            for block in BLOCKS[length]:
                total = None
                for d, base in block:
                    code = codes[d]
                    half = (code >> 5) & 1
                    flip = (code >> 6) & 1
                    active = (code >> 7) == 1
                    start = half * length + flip * (length - 1)
                    if d < 4:
                        cell = start + (1 - 2 * flip) * (lane - base)
                        inside = (lane >= base) & (lane < base + length)
                    else:
                        cell = start + jnp.zeros_like(lane)
                        inside = lane == base
                    cell = jnp.where(inside & active, cell, -1)
                    chosen = jnp.where(source == cell, 1.0, 0.0).astype(BF16)
                    piece = dot(frame(code), chosen)
                    total = piece if total is None else total + piece
                out[row_out : row_out + channels, :] = total.astype(BF16)
                row_out += channels
            row_in += rows_in


def pick(codes, gathered, specs, targets):
    rows = sum(channels * len(BLOCKS[length]) for channels, length in specs)
    shape = jax.ShapeDtypeStruct((rows, 128), BF16)
    return pl.pallas_call(
        functools.partial(pick_kernel, specs=specs),
        out_shape=(shape,) * targets,
        in_specs=[pl.BlockSpec(memory_space=pltpu.SMEM), pl.BlockSpec(memory_space=pltpu.VMEM)],
        compiler_params=LIMIT,
        name="pick",
    )(codes, gathered)


def call(kernel, shapes, *args, stage=0):
    return pl.pallas_call(
        kernel,
        out_shape=tuple(jax.ShapeDtypeStruct(s, t) for s, t in shapes),
        scratch_shapes=[pltpu.VMEM((4, stage, 128), BF16)] if stage else [],
        compiler_params=LIMIT,
    )(*[in_vmem(x) for x in args])


def start_kernel(x_ref, film_ref, a_ref, slots, stage):
    a = activate(x_ref[...].astype(F32), columns_of(film_ref[...]))
    a_ref[...] = a
    put_slots(stage, 0, frame_64(a, ones_at((4096, 128), 1, side_cell)), 64)
    send_slots(stage, slots)


def finish_1(base, x, own, down, up, w, we, cm, wet, c64, x32t, film, skip_ref, a_ref, slots, skip_frame_ref, stage):
    halo = halo_of(own, down, up, 0, 32, 3).astype(BF16)
    first = x[...].astype(F32) + with_halo_64(base[...], halo, w[...], we[...], cm[...])
    skip = first.astype(BF16)
    skip_ref[...] = skip
    a = activate(by_chunks(first, c64[...]), film_of(film, 2))
    a_ref[...] = a
    put_slots(stage, 0, dot(a, x32t[...]).astype(BF16), 32)
    send_slots(stage, slots)
    skip_frame_ref[...] = frame_64(skip, wet[...])


def finish_2(base, own, down, up, w, x32, c32, x32t, x16t, film, skip_ref, a_ref, slots, skip_frame_ref, stage):
    halo = halo_of(own, down, up, 0, 32, 2).astype(BF16)
    second = with_halo(base[...], halo, w[...], 32, x32[...])
    skip = second.astype(BF16)
    skip_ref[...] = skip
    a = activate(by_chunks(second, c32[...]), film_of(film, 3))
    a_ref[...] = a
    put_slots(stage, 0, dot(a, x16t[...]).astype(BF16), 16)
    send_slots(stage, slots)
    skip_frame_ref[...] = dot(skip, x32t[...]).astype(BF16)


def finish_3(base, own, down, up, w, x16, x16t, film, third_ref, a_ref, slots, stage):
    halo = halo_of(own, down, up, 0, 64, 1).astype(BF16)
    third = with_halo(base[...], halo, w[...], 16, x16[...])
    third_ref[...] = third
    a = activate(third, film_of(film, 4))
    a_ref[...] = a
    put_slots(stage, 0, dot(a, x16t[...]).astype(BF16), 16)
    send_slots(stage, slots)


def finish_4(base, third, own, down, up, w, x16, x16t, r32, skip, skip_frame, film, a_ref, slots, stage):
    halo = halo_of(own, down, up, 0, 128, 1).astype(BF16)
    fourth = third[...] + with_halo(base[...], halo, w[...], 16, x16[...])
    put_slots(stage, 0, dot(fourth.astype(BF16), x16t[...]).astype(BF16), 16)
    put_slots(stage, 32, skip_frame[...], 32)
    send_slots(stage, slots)
    joined = jnp.concatenate([by_chunks(fourth, r32[...]), skip[...].astype(F32)], axis=0)
    a_ref[...] = activate(joined, film_of(film, 5))


def finish_5(base, own, down, up, w, x32, x32t, double, r64, skip, skip_frame, film, a_ref, slots, stage):
    coarse = dot(halo_of(own, down, up, 0, 128, 1).astype(BF16), double[...])
    halo = activate(jnp.concatenate([coarse, halo_of(own, down, up, 128, 64, 2)], axis=0), film_of(film, 5))
    fifth = with_halo(base[...], halo, w[...], 32, x32[...])
    put_slots(stage, 0, dot(fifth.astype(BF16), x32t[...]).astype(BF16), 32)
    put_slots(stage, 32, skip_frame[...], 64)
    send_slots(stage, slots)
    joined = jnp.concatenate([by_chunks(fifth, r64[...]), skip[...].astype(F32)], axis=0)
    a_ref[...] = activate(joined, film_of(film, 6))


def finish_6(base, own, down, up, w, we, cm, double, skip, film, out_ref):
    coarse = dot(halo_of(own, down, up, 0, 64, 2).astype(BF16), double[...])
    halo = activate(jnp.concatenate([coarse, halo_of(own, down, up, 128, 32, 3)], axis=0), film_of(film, 6))
    total = with_halo_64(base[...], halo, w[...], we[...], cm[...])
    out_ref[...] = (skip[...].astype(F32) + total).astype(BF16)


def border_cell(k, length):
    cells = length * length
    part, place = k // length, k % length
    cell = jnp.where(part == 0, place, jnp.where(part == 1, cells - length + place, -1))
    cell = jnp.where(part == 2, place * length, jnp.where(part == 3, place * length + length - 1, cell))
    end = 4 * length
    cell = jnp.where(k == end, 0, jnp.where(k == end + 1, length - 1, cell))
    return jnp.where(k == end + 2, cells - length, jnp.where(k == end + 3, cells - 1, cell))


def chunk_lane(lane, length):
    return (lane // length // 2) * (length // 2) + (lane % length) // 2


def double_lane(lane, length):
    end = 4 * length
    half = (lane // length) * (length // 2) + (lane % length) // 2
    return jnp.where(lane < end, half, jnp.where(lane < end + 4, lane - 2 * length, -1))


def side_cell(k):
    return jnp.where(k < 64, k * 64, (k - 64) * 64 + 63)


def corner_lane(k):
    return jnp.where(k == 0, 0, jnp.where(k == 1, 63, jnp.where(k == 2, 64, jnp.where(k == 3, 127, -1))))


def ones_at(shape, axis, function, value=1.0):
    own = [1, 1]
    own[axis] = shape[axis]
    wanted = function(lax.broadcasted_iota(jnp.int32, tuple(own), axis))
    other = lax.broadcasted_iota(jnp.int32, shape, 1 - axis)
    return jnp.where(other == wanted, value, 0.0).astype(BF16)


MATRICES = {
    "we": ((128, 4096), 0, side_cell, 1.0),
    "wet": ((4096, 128), 1, side_cell, 1.0),
    "cm": ((128, 128), 0, corner_lane, 1.0),
    "c64": ((512, 128), 0, lambda k: chunk_lane(k, 64), 0.25),
    "x32t": ((1024, 128), 1, lambda k: border_cell(k, 32), 1.0),
    "x32": ((256, 1024), 0, lambda k: border_cell(k, 32), 1.0),
    "c32": ((512, 128), 0, lambda k: chunk_lane(k, 32), 0.25),
    "x16t": ((256, 128), 1, lambda k: jnp.where(k < 64, border_cell(k, 16), -1), 1.0),
    "x16": ((128, 256), 0, lambda k: border_cell(k, 16), 1.0),
    "r32": ((128, 512), 1, lambda k: chunk_lane(k, 32), 1.0),
    "r64": ((128, 512), 1, lambda k: chunk_lane(k, 64), 1.0),
    "double32": ((128, 256), 1, lambda k: double_lane(k, 32), 1.0),
    "double64": ((256, 384), 1, lambda k: double_lane(k, 64), 1.0),
}


def matrices_kernel(*outs):
    for out, (shape, axis, function, value) in zip(outs, MATRICES.values()):
        out[...] = ones_at(shape, axis, function, value)


def columns_of(film):
    channels = film.shape[1]
    square = [lax.broadcasted_iota(jnp.int32, (channels, channels), dim) for dim in (0, 1)]
    same = square[0] == square[1]
    columns = [jnp.sum(jnp.where(same, film[k : k + 1, :], 0.0), axis=1, keepdims=True) for k in (0, 1)]
    return jnp.concatenate(columns, axis=1)


def prepare_kernel(*refs):
    films, weights, film_out, outs = refs[:6], refs[6:12], refs[12], refs[13:]
    for film, (first, last) in zip(films, FILM_ROWS.values()):
        film_out[first:last, :] = columns_of(film[...])
    for weight, out in zip(weights, outs):
        out_channels = weight.shape[0]
        channels = weight.shape[1] // 9
        for t in range(9):
            out[t * out_channels : (t + 1) * out_channels, :] = weight[:, t * channels : (t + 1) * channels]


NEAR_RELAY = {p: p for p in (0, 3, 4, 7, 24, 27, 28, 31)}
NEAR_RELAY |= {1: 2, 2: 10, 8: 11, 6: 5, 5: 13, 15: 12, 25: 26, 26: 18, 16: 19, 30: 29, 29: 21, 23: 20}
FAR_RELAY = {0: 26, 1: 27, 2: 18, 3: 19, 8: 24, 16: 0, 24: 2, 25: 3, 26: 10, 27: 11}
FAR_RELAY |= {7: 29, 6: 28, 5: 21, 4: 20, 15: 31, 23: 7, 31: 5, 30: 4, 29: 13, 28: 12}


def other_face(face, kind):
    return face ^ 1 if kind == 0 else (face + 1 if face % 2 else face - 1) % 8


def face_moves(kind):
    moves = []
    for face in range(8):
        far = kind == 1 and face % 4 in (0, 3)
        for target, relay in (FAR_RELAY if far else NEAR_RELAY).items():
            moves.append((face * 32 + relay, other_face(face, kind) * 32 + target))
    return moves


def inverse(relays):
    targets = np.full(32, -1)
    for target, relay in relays.items():
        targets[relay] = target
    return targets


def link_codes(link_patch, link_shift, link_turn):
    packed = TURN_EDGE[:, READ_EDGE] * 2 + (TURN_FLIP[:, READ_EDGE] ^ READ_END[None, :])
    choice = jnp.zeros(link_turn.shape, jnp.int32)
    for turn in range(4):
        choice = jnp.where(link_turn == turn, jnp.asarray(packed[turn], jnp.int32), choice)
    edge, flip = choice // 2, choice % 2
    row, column = link_patch // 8, link_patch % 8
    outer = jnp.where(row == 0, 0, jnp.where(row == 3, 1, jnp.where(column == 0, 2, 3)))
    cell_row = jnp.where(edge < 2, edge, flip)
    cell_column = jnp.where(edge < 2, flip, edge - 2)
    in_first = jnp.where(outer < 2, cell_row == outer, cell_column == outer - 2)
    is_corner = jnp.asarray(np.arange(8) >= 4)
    half = jnp.where(is_corner, jnp.where(in_first, 0, 1), jnp.where(edge == outer, 0, 1))
    corner_flip = jnp.where(in_first & (outer < 2), cell_column, cell_row)
    inside = link_shift == 0
    half = jnp.where(inside, 1, half)
    flip = jnp.where(is_corner, jnp.where(inside, cell_column, corner_flip), flip)
    flat = (link_patch + half * 32 + flip * 64 + (link_shift + 1) * 128).reshape(256, 8)
    face = lax.axis_index("face")
    patch = lax.axis_index("patch")
    odd = face % 2
    this = np.arange(32) == patch
    near = jnp.sum(jnp.where(this, jnp.asarray(inverse(NEAR_RELAY), jnp.int32), 0))
    far = jnp.sum(jnp.where(this, jnp.asarray(inverse(FAR_RELAY), jnp.int32), 0))
    far = jnp.where((face % 4 == 0) | (face % 4 == 3), far, near)
    places = [
        (face, patch, 1),
        (face + 1 - 2 * odd, near, 2 * odd),
        ((face + 7 + 2 * odd) % 8, far, 2 - 2 * odd),
    ]
    rows = []
    for of_face, of_patch, shift in places:
        chosen = lax.dynamic_slice(flat, (of_face * 32 + jnp.maximum(of_patch, 0), 0), (1, 8))
        active = (chosen // 128 == shift) & (of_patch >= 0)
        rows.append(chosen % 128 + jnp.where(active, 128, 0))
    return jnp.concatenate(rows, axis=0).reshape(24)


def body(
    features,
    film_first,
    weight_first,
    film_second,
    weight_second,
    film_third,
    weight_third,
    film_fourth,
    weight_fourth,
    film_fifth,
    weight_fifth,
    film_sixth,
    weight_sixth,
    link_patch,
    link_shift,
    link_turn,
):
    x = features[:, 0, :]
    codes = link_codes(link_patch, link_shift, link_turn)
    films = (film_first, film_second, film_third, film_fourth, film_fifth, film_sixth)
    weights = (weight_first, weight_second, weight_third, weight_fourth, weight_fifth, weight_sixth)
    rows = [((9 * w.shape[0], w.shape[1] // 9), BF16) for w in weights]
    film, w1, w2, w3, w4, w5, w6 = call(prepare_kernel, [((544, 2), F32)] + rows, *films, *weights)
    made = call(matrices_kernel, [(entry[0], BF16) for entry in MATRICES.values()])
    we, wet, cm, c64, x32t, x32, c32, x16t, x16, r32, r64, double32, double64 = made
    near_moves = face_moves(0)
    far_moves = face_moves(1)

    def exchange(slots, specs):
        gathered = lax.all_to_all(slots, "patch", split_axis=0, concat_axis=0, tiled=True)
        gathered = in_vmem(gathered)
        for_near, for_far = pick(codes[8:], gathered, specs, 2)
        from_far = lax.ppermute(for_far, ("face", "patch"), far_moves)
        from_near = lax.ppermute(for_near, ("face", "patch"), near_moves)
        (own,) = pick(codes[:8], gathered, specs, 1)
        return own, from_near, from_far

    a1, f1 = call(start_kernel, [((32, 4096), BF16), ((32, 32, 128), BF16)], x, film_first, stage=32)
    h = exchange(f1, ((32, 64),))
    base = main_conv(a1, w1, 64)
    skip_fine, a2, f2, fine_frame = call(
        finish_1,
        [((32, 4096), BF16), ((32, 1024), BF16), ((32, 16, 128), BF16), ((32, 256), BF16)],
        base, x, *h, w1, we, cm, wet, c64, x32t, film,
        stage=16,
    )
    h = exchange(f2, ((32, 32),))
    base = main_conv(a2, w2, 32)
    skip_middle, a3, f3, middle_frame = call(
        finish_2,
        [((64, 1024), BF16), ((64, 256), BF16), ((32, 16, 128), BF16), ((64, 128), BF16)],
        base, *h, w2, x32, c32, x32t, x16t, film,
        stage=16,
    )
    h = exchange(f3, ((64, 16),))
    base = main_conv(a3, w3, 16)
    third, a4, f4 = call(
        finish_3,
        [((128, 256), F32), ((128, 256), BF16), ((32, 32, 128), BF16)],
        base, *h, w3, x16, x16t, film,
        stage=32,
    )
    h = exchange(f4, ((128, 16),))
    base = main_conv(a4, w4, 16)
    a5, f5 = call(
        finish_4,
        [((192, 1024), BF16), ((32, 64, 128), BF16)],
        base, third, *h, w4, x16, x16t, r32, skip_middle, middle_frame, film,
        stage=64,
    )
    h = exchange(f5, ((128, 16), (64, 32)))
    base = main_conv(a5, w5, 32)
    a6, f6 = call(
        finish_5,
        [((96, 4096), BF16), ((32, 64, 128), BF16)],
        base, *h, w5, x32, x32t, double32, r64, skip_fine, fine_frame, film,
        stage=64,
    )
    h = exchange(f6, ((64, 32), (32, 64)))
    base = main_conv(a6, w6, 64)
    (result,) = call(
        finish_6,
        [((32, 4096), BF16)],
        base, *h, w6, we, cm, double64, skip_fine, film,
    )
    return result[:, None, :]


def solution(mesh):
    in_specs = (P(None, "face", "patch"),) + (P(),) * 15
    out_specs = P(None, "face", "patch")
    return jax.shard_map(body, mesh=mesh, in_specs=in_specs, out_specs=out_specs, check_vma=False)
```

```python
import functools

import jax
import jax.numpy as jnp
import numpy as np
from jax import lax
from jax.experimental import pallas as pl
from jax.experimental.pallas import tpu as pltpu
from jax.sharding import PartitionSpec as P

EPSILON = 1e-05
FLOOR_SQUARE = 0.5
F32 = jnp.float32
BF16 = jnp.bfloat16
LIMIT = pltpu.CompilerParams(vmem_limit_bytes=24 * 1024 * 1024)
FILM_ROWS = {1: (0, 32), 2: (32, 64), 3: (64, 128), 4: (128, 256), 5: (256, 448), 6: (448, 544)}
TURN_EDGE = np.array([[0, 1, 2, 3], [3, 2, 0, 1], [1, 0, 3, 2], [2, 3, 1, 0]])
TURN_FLIP = np.array([[0, 0, 0, 0], [0, 0, 1, 1], [1, 1, 1, 1], [1, 1, 0, 0]])
READ_EDGE = np.array([1, 0, 3, 2, 1, 1, 0, 0])
READ_END = np.array([0, 0, 0, 0, 1, 0, 1, 0])
CORNERS = [(4, 0), (5, 1), (6, 2), (7, 3)]
BLOCKS = {
    64: [[(0, 0), (1, 64)], [(2, 0), (3, 64)], CORNERS],
    32: [[(0, 0), (1, 32), (2, 64), (3, 96)], CORNERS],
    16: [[(0, 0), (1, 16), (2, 32), (3, 48), (4, 64), (5, 65), (6, 66), (7, 67)]],
}


def dot(a, b):
    return jnp.dot(a, b, preferred_element_type=F32)


def in_vmem(x):
    return pltpu.with_memory_space_constraint(x, pltpu.VMEM)


def lanes_of(width):
    return lax.broadcasted_iota(jnp.int32, (1, width), 1)


def halves(x):
    high = x.astype(BF16)
    return high, (x - high.astype(F32)).astype(BF16)


def activate(values, film):
    mean_square = jnp.mean(values * values, axis=0, keepdims=True)
    if values.shape[0] >= 64:
        inverse = lax.rsqrt(mean_square + EPSILON)
    else:
        inverse = lax.rsqrt(jnp.maximum(mean_square, FLOOR_SQUARE))
    shaped = values * inverse * (1.0 + film[:, 0:1]) + film[:, 1:2]
    return (shaped / (1.0 + jnp.exp(-shaped))).astype(BF16)


def film_of(ref, index):
    first, last = FILM_ROWS[index]
    return ref[first:last, :]


def by_chunks(x, matrix):
    channels = x.shape[0]
    run = matrix.shape[0]
    count = x.shape[1] // run
    stacked = jnp.concatenate([x[:, run * k : run * (k + 1)] for k in range(count)], axis=0)
    high, low = halves(stacked)
    result = dot(high, matrix) + dot(low, matrix)
    return jnp.concatenate([result[channels * k : channels * (k + 1)] for k in range(count)], axis=1)


def frame_64(a, west_east_t):
    cells = a.shape[1]
    upper = jnp.where(lanes_of(128) < 64, a[:, :128].astype(F32), a[:, cells - 128 :].astype(F32))
    return jnp.concatenate([upper, dot(a, west_east_t)], axis=1).astype(BF16)


def put_slots(stage, first, frame, length):
    groups = 64 // length
    rows = frame.shape[0] // groups
    patch = lax.axis_index("patch")
    row, column = patch // 8, patch % 8
    outer = jnp.where(row == 0, 0, jnp.where(row == 3, 1, jnp.where(column == 0, 2, 3)))
    source = lax.broadcasted_iota(jnp.int32, (frame.shape[1], 128), 0)

    def placed(edge, half):
        total = None
        for group in range(groups):
            place = lanes_of(128) - (2 * group + half) * length
            wanted = jnp.where((place >= 0) & (place < length), edge * length + place, -1)
            chosen = jnp.where(source == wanted, 1.0, 0.0).astype(BF16)
            piece = dot(frame[group * rows : (group + 1) * rows], chosen)
            total = piece if total is None else total + piece
        return total

    shared = placed(outer, 0)
    for edge in range(4):
        stage[edge, first : first + rows, :] = (shared + placed(edge, 1)).astype(BF16)


def send_slots(stage, out):
    patch = lax.axis_index("patch")
    row, column = patch // 8, patch % 8
    second = jnp.where(column == 0, 2, 3)
    for target in range(32):
        down = target // 8 - row
        right = target % 8 - column
        near = (down >= -1) & (down <= 1) & (right >= -1) & (right <= 1) & (target != patch)
        across = jnp.where(right > 0, 3, 2)
        inner = jnp.where(down > 0, 1, jnp.where(down < 0, 0, across))
        out[target] = stage[jnp.where(near, inner, second)]


def halo_of(own, down, up, first, channels, blocks):
    rows = slice(first, first + channels * blocks)
    packed = own[rows, :].astype(F32) + down[rows, :].astype(F32) + up[rows, :].astype(F32)
    return jnp.concatenate([packed[channels * k : channels * (k + 1)] for k in range(blocks)], axis=1)


def expand(z, matrix):
    high, low = halves(z)
    both = dot(jnp.concatenate([high, low], axis=0), matrix)
    return both[: z.shape[0]] + both[z.shape[0] :]


def border_sums(halo, weight, length):
    products = dot(weight, halo)
    out_channels = weight.shape[0] // 9
    width = halo.shape[1]

    def tap(u, v):
        t = 3 * (u + 1) + v + 1
        return products[t * out_channels : (t + 1) * out_channels]

    lane = lanes_of(width)
    part = lane // length
    place = lane % length

    def along(step):
        return jnp.where(
            part == 0,
            tap(-1, step),
            jnp.where(part == 1, tap(1, step), jnp.where(part == 2, tap(step, -1), tap(step, 1))),
        )

    end = 4 * length
    corner = jnp.where(lane == end, tap(-1, -1), 0.0)
    corner = jnp.where(lane == end + 1, tap(-1, 1), corner)
    corner = jnp.where(lane == end + 2, tap(1, -1), corner)
    corner = jnp.where(lane == end + 3, tap(1, 1), corner)
    edge = part < 4
    before = jnp.where(edge & (place != 0), pltpu.roll(along(-1), 1, 1), 0.0)
    after = jnp.where(edge & (place != length - 1), pltpu.roll(along(1), width - 1, 1), 0.0)
    return jnp.where(edge, along(0), corner) + before + after


def with_halo_64(base, halo, weight, west_east, corner_map):
    sums = border_sums(halo, weight, 64)
    rows = sums[:, :128] + expand(sums[:, 256:], corner_map)
    total = base + expand(sums[:, 128:256], west_east)
    cells = total.shape[1]
    low = lanes_of(128) < 64
    top = total[:, :128] + jnp.where(low, rows, 0.0)
    bottom = total[:, cells - 128 :] + jnp.where(low, 0.0, rows)
    return jnp.concatenate([top, total[:, 128 : cells - 128], bottom], axis=1)


def with_halo(base, halo, weight, length, matrix):
    return base + expand(border_sums(halo, weight, length), matrix)


def main_kernel(a_ref, w_ref, out_ref, products, *, length):
    products[...] = dot(w_ref[...], a_ref[...])
    out_channels, cells = out_ref.shape
    lane = lanes_of(cells)
    place = lane % length

    def tap(u, v):
        t = 3 * (u + 1) + v + 1
        return products[t * out_channels : (t + 1) * out_channels, :]

    def column(v):
        above = jnp.where(lane < length, 0.0, pltpu.roll(tap(-1, v), length, 1))
        below = jnp.where(lane >= cells - length, 0.0, pltpu.roll(tap(1, v), cells - length, 1))
        return tap(0, v) + above + below

    total = column(0)
    total += jnp.where(place == 0, 0.0, pltpu.roll(column(-1), 1, 1))
    total += jnp.where(place == length - 1, 0.0, pltpu.roll(column(1), cells - 1, 1))
    out_ref[...] = total


def main_conv(a, weight, length):
    taps_out = weight.shape[0]
    cells = a.shape[1]
    return pl.pallas_call(
        functools.partial(main_kernel, length=length),
        out_shape=jax.ShapeDtypeStruct((taps_out // 9, cells), F32),
        scratch_shapes=[pltpu.VMEM((taps_out, cells), F32)],
        cost_estimate=pl.CostEstimate(
            flops=2 * taps_out * weight.shape[1] * cells * 8, bytes_accessed=a.size * 2 + taps_out * cells, transcendentals=0
        ),
        compiler_params=LIMIT,
        name="main_conv",
    )(in_vmem(a), in_vmem(weight))


def pick_kernel(code_ref, gathered, *outs, specs):
    for target, out in enumerate(outs):
        codes = [code_ref[target * 8 + d] for d in range(8)]
        row_out = 0
        row_in = 0
        for channels, length in specs:
            groups = 64 // length
            rows_in = channels // groups
            lane = lanes_of(128)
            source = lax.broadcasted_iota(jnp.int32, (128, 128), 0) & (2 * length - 1)

            def frame(code):
                rows = gathered[code & 31, row_in : row_in + rows_in, :]
                if groups == 1:
                    return rows
                wide = rows.astype(F32)
                split = [jnp.where(lane // (2 * length) == group, wide, 0.0) for group in range(groups)]
                return jnp.concatenate(split, axis=0).astype(BF16)

            for block in BLOCKS[length]:
                total = None
                for d, base in block:
                    code = codes[d]
                    half = (code >> 5) & 1
                    flip = (code >> 6) & 1
                    active = (code >> 7) == 1
                    start = half * length + flip * (length - 1)
                    if d < 4:
                        cell = start + (1 - 2 * flip) * (lane - base)
                        inside = (lane >= base) & (lane < base + length)
                    else:
                        cell = start + jnp.zeros_like(lane)
                        inside = lane == base
                    cell = jnp.where(inside & active, cell, -1)
                    chosen = jnp.where(source == cell, 1.0, 0.0).astype(BF16)
                    piece = dot(frame(code), chosen)
                    total = piece if total is None else total + piece
                out[row_out : row_out + channels, :] = total.astype(BF16)
                row_out += channels
            row_in += rows_in


def pick(codes, gathered, specs, targets):
    rows = sum(channels * len(BLOCKS[length]) for channels, length in specs)
    shape = jax.ShapeDtypeStruct((rows, 128), BF16)
    return pl.pallas_call(
        functools.partial(pick_kernel, specs=specs),
        out_shape=(shape,) * targets,
        in_specs=[pl.BlockSpec(memory_space=pltpu.SMEM), pl.BlockSpec(memory_space=pltpu.VMEM)],
        compiler_params=LIMIT,
        name="pick",
    )(codes, gathered)


def call(kernel, shapes, *args, stage=0):
    return pl.pallas_call(
        kernel,
        out_shape=tuple(jax.ShapeDtypeStruct(s, t) for s, t in shapes),
        scratch_shapes=[pltpu.VMEM((4, stage, 128), BF16)] if stage else [],
        compiler_params=LIMIT,
    )(*[in_vmem(x) for x in args])


def start_kernel(x_ref, film_ref, a_ref, slots, stage):
    a = activate(x_ref[...].astype(F32), columns_of(film_ref[...]))
    a_ref[...] = a
    put_slots(stage, 0, frame_64(a, ones_at((4096, 128), 1, side_cell)), 64)
    send_slots(stage, slots)


def finish_1(base, x, own, down, up, w, we, cm, wet, c64, x32t, film, skip_ref, a_ref, slots, skip_frame_ref, stage):
    halo = halo_of(own, down, up, 0, 32, 3).astype(BF16)
    first = x[...].astype(F32) + with_halo_64(base[...], halo, w[...], we[...], cm[...])
    skip = first.astype(BF16)
    skip_ref[...] = skip
    a = activate(by_chunks(first, c64[...]), film_of(film, 2))
    a_ref[...] = a
    put_slots(stage, 0, dot(a, x32t[...]).astype(BF16), 32)
    send_slots(stage, slots)
    skip_frame_ref[...] = frame_64(skip, wet[...])


def finish_2(base, own, down, up, w, x32, c32, x32t, x16t, film, skip_ref, a_ref, slots, skip_frame_ref, stage):
    halo = halo_of(own, down, up, 0, 32, 2).astype(BF16)
    second = with_halo(base[...], halo, w[...], 32, x32[...])
    skip = second.astype(BF16)
    skip_ref[...] = skip
    a = activate(by_chunks(second, c32[...]), film_of(film, 3))
    a_ref[...] = a
    put_slots(stage, 0, dot(a, x16t[...]).astype(BF16), 16)
    send_slots(stage, slots)
    skip_frame_ref[...] = dot(skip, x32t[...]).astype(BF16)


def finish_3(base, own, down, up, w, x16, x16t, film, third_ref, a_ref, slots, stage):
    halo = halo_of(own, down, up, 0, 64, 1).astype(BF16)
    third = with_halo(base[...], halo, w[...], 16, x16[...])
    third_ref[...] = third
    a = activate(third, film_of(film, 4))
    a_ref[...] = a
    put_slots(stage, 0, dot(a, x16t[...]).astype(BF16), 16)
    send_slots(stage, slots)


def finish_4(base, third, own, down, up, w, x16, x16t, r32, skip, skip_frame, film, a_ref, slots, stage):
    halo = halo_of(own, down, up, 0, 128, 1).astype(BF16)
    fourth = third[...] + with_halo(base[...], halo, w[...], 16, x16[...])
    put_slots(stage, 0, dot(fourth.astype(BF16), x16t[...]).astype(BF16), 16)
    put_slots(stage, 32, skip_frame[...], 32)
    send_slots(stage, slots)
    joined = jnp.concatenate([by_chunks(fourth, r32[...]), skip[...].astype(F32)], axis=0)
    a_ref[...] = activate(joined, film_of(film, 5))


def finish_5(base, own, down, up, w, x32, x32t, double, r64, skip, skip_frame, film, a_ref, slots, stage):
    coarse = dot(halo_of(own, down, up, 0, 128, 1).astype(BF16), double[...])
    halo = activate(jnp.concatenate([coarse, halo_of(own, down, up, 128, 64, 2)], axis=0), film_of(film, 5))
    fifth = with_halo(base[...], halo, w[...], 32, x32[...])
    put_slots(stage, 0, dot(fifth.astype(BF16), x32t[...]).astype(BF16), 32)
    put_slots(stage, 32, skip_frame[...], 64)
    send_slots(stage, slots)
    joined = jnp.concatenate([by_chunks(fifth, r64[...]), skip[...].astype(F32)], axis=0)
    a_ref[...] = activate(joined, film_of(film, 6))


def finish_6(base, own, down, up, w, we, cm, double, skip, film, out_ref):
    coarse = dot(halo_of(own, down, up, 0, 64, 2).astype(BF16), double[...])
    halo = activate(jnp.concatenate([coarse, halo_of(own, down, up, 128, 32, 3)], axis=0), film_of(film, 6))
    total = with_halo_64(base[...], halo, w[...], we[...], cm[...])
    out_ref[...] = (skip[...].astype(F32) + total).astype(BF16)


def border_cell(k, length):
    cells = length * length
    part, place = k // length, k % length
    cell = jnp.where(part == 0, place, jnp.where(part == 1, cells - length + place, -1))
    cell = jnp.where(part == 2, place * length, jnp.where(part == 3, place * length + length - 1, cell))
    end = 4 * length
    cell = jnp.where(k == end, 0, jnp.where(k == end + 1, length - 1, cell))
    return jnp.where(k == end + 2, cells - length, jnp.where(k == end + 3, cells - 1, cell))


def chunk_lane(lane, length):
    return (lane // length // 2) * (length // 2) + (lane % length) // 2


def double_lane(lane, length):
    end = 4 * length
    half = (lane // length) * (length // 2) + (lane % length) // 2
    return jnp.where(lane < end, half, jnp.where(lane < end + 4, lane - 2 * length, -1))


def side_cell(k):
    return jnp.where(k < 64, k * 64, (k - 64) * 64 + 63)


def corner_lane(k):
    return jnp.where(k == 0, 0, jnp.where(k == 1, 63, jnp.where(k == 2, 64, jnp.where(k == 3, 127, -1))))


def ones_at(shape, axis, function, value=1.0):
    own = [1, 1]
    own[axis] = shape[axis]
    wanted = function(lax.broadcasted_iota(jnp.int32, tuple(own), axis))
    other = lax.broadcasted_iota(jnp.int32, shape, 1 - axis)
    return jnp.where(other == wanted, value, 0.0).astype(BF16)


MATRICES = {
    "we": ((128, 4096), 0, side_cell, 1.0),
    "wet": ((4096, 128), 1, side_cell, 1.0),
    "cm": ((128, 128), 0, corner_lane, 1.0),
    "c64": ((512, 128), 0, lambda k: chunk_lane(k, 64), 0.25),
    "x32t": ((1024, 128), 1, lambda k: border_cell(k, 32), 1.0),
    "x32": ((256, 1024), 0, lambda k: border_cell(k, 32), 1.0),
    "c32": ((512, 128), 0, lambda k: chunk_lane(k, 32), 0.25),
    "x16t": ((256, 128), 1, lambda k: jnp.where(k < 64, border_cell(k, 16), -1), 1.0),
    "x16": ((128, 256), 0, lambda k: border_cell(k, 16), 1.0),
    "r32": ((128, 512), 1, lambda k: chunk_lane(k, 32), 1.0),
    "r64": ((128, 512), 1, lambda k: chunk_lane(k, 64), 1.0),
    "double32": ((128, 256), 1, lambda k: double_lane(k, 32), 1.0),
    "double64": ((256, 384), 1, lambda k: double_lane(k, 64), 1.0),
}


def matrices_kernel(*outs):
    for out, (shape, axis, function, value) in zip(outs, MATRICES.values()):
        out[...] = ones_at(shape, axis, function, value)


def columns_of(film):
    channels = film.shape[1]
    square = [lax.broadcasted_iota(jnp.int32, (channels, channels), dim) for dim in (0, 1)]
    same = square[0] == square[1]
    columns = [jnp.sum(jnp.where(same, film[k : k + 1, :], 0.0), axis=1, keepdims=True) for k in (0, 1)]
    return jnp.concatenate(columns, axis=1)


def prepare_kernel(*refs):
    films, weights, film_out, outs = refs[:6], refs[6:12], refs[12], refs[13:]
    for film, (first, last) in zip(films, FILM_ROWS.values()):
        film_out[first:last, :] = columns_of(film[...])
    for weight, out in zip(weights, outs):
        out_channels = weight.shape[0]
        channels = weight.shape[1] // 9
        for t in range(9):
            out[t * out_channels : (t + 1) * out_channels, :] = weight[:, t * channels : (t + 1) * channels]


def swaps(left):
    pairs = {}
    for one, other in left:
        for a, b in ((one, other), (other, one)):
            pairs[a] = b
            pairs[a // 8 * 8 + 7 - a % 8] = b // 8 * 8 + 7 - b % 8
    return pairs


NEAR_RELAY = {p: p for p in range(32)} | swaps([(1, 11), (8, 10), (16, 18), (25, 19)])
FAR_RELAY = swaps([(0, 24), (2, 26), (3, 27), (1, 19), (25, 11), (8, 18), (16, 10), (9, 17)])


def other_face(face, kind):
    return face ^ 1 if kind == 0 else (face + 1 if face % 2 else face - 1) % 8


def face_moves(kind):
    moves = []
    for face in range(8):
        far = kind == 1 and face % 4 in (0, 3)
        for target, relay in (FAR_RELAY if far else NEAR_RELAY).items():
            moves.append((face * 32 + relay, other_face(face, kind) * 32 + target))
    return moves


def inverse(relays):
    targets = np.full(32, -1)
    for target, relay in relays.items():
        targets[relay] = target
    return targets


def link_codes(link_patch, link_shift, link_turn):
    packed = TURN_EDGE[:, READ_EDGE] * 2 + (TURN_FLIP[:, READ_EDGE] ^ READ_END[None, :])
    choice = jnp.zeros(link_turn.shape, jnp.int32)
    for turn in range(4):
        choice = jnp.where(link_turn == turn, jnp.asarray(packed[turn], jnp.int32), choice)
    edge, flip = choice // 2, choice % 2
    row, column = link_patch // 8, link_patch % 8
    outer = jnp.where(row == 0, 0, jnp.where(row == 3, 1, jnp.where(column == 0, 2, 3)))
    cell_row = jnp.where(edge < 2, edge, flip)
    cell_column = jnp.where(edge < 2, flip, edge - 2)
    in_first = jnp.where(outer < 2, cell_row == outer, cell_column == outer - 2)
    is_corner = jnp.asarray(np.arange(8) >= 4)
    half = jnp.where(is_corner, jnp.where(in_first, 0, 1), jnp.where(edge == outer, 0, 1))
    corner_flip = jnp.where(in_first & (outer < 2), cell_column, cell_row)
    inside = link_shift == 0
    half = jnp.where(inside, 1, half)
    flip = jnp.where(is_corner, jnp.where(inside, cell_column, corner_flip), flip)
    flat = (link_patch + half * 32 + flip * 64 + (link_shift + 1) * 128).reshape(256, 8)
    face = lax.axis_index("face")
    patch = lax.axis_index("patch")
    odd = face % 2
    this = np.arange(32) == patch
    near = jnp.sum(jnp.where(this, jnp.asarray(inverse(NEAR_RELAY), jnp.int32), 0))
    far = jnp.sum(jnp.where(this, jnp.asarray(inverse(FAR_RELAY), jnp.int32), 0))
    far = jnp.where((face % 4 == 0) | (face % 4 == 3), far, near)
    places = [
        (face, patch, 1),
        (face + 1 - 2 * odd, near, 2 * odd),
        ((face + 7 + 2 * odd) % 8, far, 2 - 2 * odd),
    ]
    rows = []
    for of_face, of_patch, shift in places:
        chosen = lax.dynamic_slice(flat, (of_face * 32 + jnp.maximum(of_patch, 0), 0), (1, 8))
        active = (chosen // 128 == shift) & (of_patch >= 0)
        rows.append(chosen % 128 + jnp.where(active, 128, 0))
    return jnp.concatenate(rows, axis=0).reshape(24)


def body(
    features,
    film_first,
    weight_first,
    film_second,
    weight_second,
    film_third,
    weight_third,
    film_fourth,
    weight_fourth,
    film_fifth,
    weight_fifth,
    film_sixth,
    weight_sixth,
    link_patch,
    link_shift,
    link_turn,
):
    x = features[:, 0, :]
    codes = link_codes(link_patch, link_shift, link_turn)
    films = (film_first, film_second, film_third, film_fourth, film_fifth, film_sixth)
    weights = (weight_first, weight_second, weight_third, weight_fourth, weight_fifth, weight_sixth)
    rows = [((9 * w.shape[0], w.shape[1] // 9), BF16) for w in weights]
    film, w1, w2, w3, w4, w5, w6 = call(prepare_kernel, [((544, 2), F32)] + rows, *films, *weights)
    made = call(matrices_kernel, [(entry[0], BF16) for entry in MATRICES.values()])
    we, wet, cm, c64, x32t, x32, c32, x16t, x16, r32, r64, double32, double64 = made
    near_moves = face_moves(0)
    far_moves = face_moves(1)

    def exchange(slots, specs):
        gathered = lax.all_to_all(slots, "patch", split_axis=0, concat_axis=0, tiled=True)
        gathered = in_vmem(gathered)
        for_near, for_far = pick(codes[8:], gathered, specs, 2)
        from_far = lax.ppermute(for_far, ("face", "patch"), far_moves)
        from_near = lax.ppermute(for_near, ("face", "patch"), near_moves)
        (own,) = pick(codes[:8], gathered, specs, 1)
        return own, from_near, from_far

    a1, f1 = call(start_kernel, [((32, 4096), BF16), ((32, 32, 128), BF16)], x, film_first, stage=32)
    h = exchange(f1, ((32, 64),))
    base = main_conv(a1, w1, 64)
    skip_fine, a2, f2, fine_frame = call(
        finish_1,
        [((32, 4096), BF16), ((32, 1024), BF16), ((32, 16, 128), BF16), ((32, 256), BF16)],
        base, x, *h, w1, we, cm, wet, c64, x32t, film,
        stage=16,
    )
    h = exchange(f2, ((32, 32),))
    base = main_conv(a2, w2, 32)
    skip_middle, a3, f3, middle_frame = call(
        finish_2,
        [((64, 1024), BF16), ((64, 256), BF16), ((32, 16, 128), BF16), ((64, 128), BF16)],
        base, *h, w2, x32, c32, x32t, x16t, film,
        stage=16,
    )
    h = exchange(f3, ((64, 16),))
    base = main_conv(a3, w3, 16)
    third, a4, f4 = call(
        finish_3,
        [((128, 256), F32), ((128, 256), BF16), ((32, 32, 128), BF16)],
        base, *h, w3, x16, x16t, film,
        stage=32,
    )
    h = exchange(f4, ((128, 16),))
    base = main_conv(a4, w4, 16)
    a5, f5 = call(
        finish_4,
        [((192, 1024), BF16), ((32, 64, 128), BF16)],
        base, third, *h, w4, x16, x16t, r32, skip_middle, middle_frame, film,
        stage=64,
    )
    h = exchange(f5, ((128, 16), (64, 32)))
    base = main_conv(a5, w5, 32)
    a6, f6 = call(
        finish_5,
        [((96, 4096), BF16), ((32, 64, 128), BF16)],
        base, *h, w5, x32, x32t, double32, r64, skip_fine, fine_frame, film,
        stage=64,
    )
    h = exchange(f6, ((64, 32), (32, 64)))
    base = main_conv(a6, w6, 64)
    (result,) = call(
        finish_6,
        [((32, 4096), BF16)],
        base, *h, w6, we, cm, double64, skip_fine, film,
    )
    return result[:, None, :]


def solution(mesh):
    in_specs = (P(None, "face", "patch"),) + (P(),) * 15
    out_specs = P(None, "face", "patch")
    return jax.shard_map(body, mesh=mesh, in_specs=in_specs, out_specs=out_specs, check_vma=False)
```

```python
import functools

import jax
import jax.numpy as jnp
import numpy as np
from jax import lax
from jax.experimental import pallas as pl
from jax.experimental.pallas import tpu as pltpu
from jax.sharding import PartitionSpec as P

EPSILON = 1e-05
FLOOR_SQUARE = 0.5
F32 = jnp.float32
BF16 = jnp.bfloat16
LIMIT = pltpu.CompilerParams(vmem_limit_bytes=24 * 1024 * 1024)
FILM_ROWS = {1: (0, 32), 2: (32, 64), 3: (64, 128), 4: (128, 256), 5: (256, 448), 6: (448, 544)}
TURN_EDGE = np.array([[0, 1, 2, 3], [3, 2, 0, 1], [1, 0, 3, 2], [2, 3, 1, 0]])
TURN_FLIP = np.array([[0, 0, 0, 0], [0, 0, 1, 1], [1, 1, 1, 1], [1, 1, 0, 0]])
READ_EDGE = np.array([1, 0, 3, 2, 1, 1, 0, 0])
READ_END = np.array([0, 0, 0, 0, 1, 0, 1, 0])
CORNERS = [(4, 0), (5, 1), (6, 2), (7, 3)]
BLOCKS = {
    64: [[(0, 0), (1, 64)], [(2, 0), (3, 64)], CORNERS],
    32: [[(0, 0), (1, 32), (2, 64), (3, 96)], CORNERS],
    16: [[(0, 0), (1, 16), (2, 32), (3, 48), (4, 64), (5, 65), (6, 66), (7, 67)]],
}


def dot(a, b):
    return jnp.dot(a, b, preferred_element_type=F32)


def in_vmem(x):
    return pltpu.with_memory_space_constraint(x, pltpu.VMEM)


def lanes_of(width):
    return lax.broadcasted_iota(jnp.int32, (1, width), 1)


def halves(x):
    high = x.astype(BF16)
    return high, (x - high.astype(F32)).astype(BF16)


def activate(values, film):
    mean_square = jnp.mean(values * values, axis=0, keepdims=True)
    if values.shape[0] >= 64:
        inverse = lax.rsqrt(mean_square + EPSILON)
    else:
        inverse = lax.rsqrt(jnp.maximum(mean_square, FLOOR_SQUARE))
    shaped = values * inverse * (1.0 + film[:, 0:1]) + film[:, 1:2]
    return (shaped / (1.0 + jnp.exp(-shaped))).astype(BF16)


def film_of(ref, index):
    first, last = FILM_ROWS[index]
    return ref[first:last, :]


def by_chunks(x, matrix):
    channels = x.shape[0]
    run = matrix.shape[0]
    count = x.shape[1] // run
    stacked = jnp.concatenate([x[:, run * k : run * (k + 1)] for k in range(count)], axis=0)
    high, low = halves(stacked)
    result = dot(high, matrix) + dot(low, matrix)
    return jnp.concatenate([result[channels * k : channels * (k + 1)] for k in range(count)], axis=1)


def frame_64(a, west_east_t):
    cells = a.shape[1]
    upper = jnp.where(lanes_of(128) < 64, a[:, :128].astype(F32), a[:, cells - 128 :].astype(F32))
    return jnp.concatenate([upper, dot(a, west_east_t)], axis=1).astype(BF16)


def put_slots(stage, first, frame, length):
    groups = 64 // length
    rows = frame.shape[0] // groups
    patch = lax.axis_index("patch")
    row, column = patch // 8, patch % 8
    outer = jnp.where(row == 0, 0, jnp.where(row == 3, 1, jnp.where(column == 0, 2, 3)))
    source = lax.broadcasted_iota(jnp.int32, (frame.shape[1], 128), 0)

    def placed(edge, half):
        total = None
        for group in range(groups):
            place = lanes_of(128) - (2 * group + half) * length
            wanted = jnp.where((place >= 0) & (place < length), edge * length + place, -1)
            chosen = jnp.where(source == wanted, 1.0, 0.0).astype(BF16)
            piece = dot(frame[group * rows : (group + 1) * rows], chosen)
            total = piece if total is None else total + piece
        return total

    shared = placed(outer, 0)
    for edge in range(4):
        stage[edge, first : first + rows, :] = (shared + placed(edge, 1)).astype(BF16)


def send_slots(stage, out):
    patch = lax.axis_index("patch")
    row, column = patch // 8, patch % 8
    second = jnp.where(column == 0, 2, 3)
    for target in range(32):
        down = target // 8 - row
        right = target % 8 - column
        near = (down >= -1) & (down <= 1) & (right >= -1) & (right <= 1) & (target != patch)
        across = jnp.where(right > 0, 3, 2)
        inner = jnp.where(down > 0, 1, jnp.where(down < 0, 0, across))
        out[target] = stage[jnp.where(near, inner, second)]


def halo_of(own, down, up, first, channels, blocks):
    rows = slice(first, first + channels * blocks)
    packed = own[rows, :].astype(F32) + down[rows, :].astype(F32) + up[rows, :].astype(F32)
    return jnp.concatenate([packed[channels * k : channels * (k + 1)] for k in range(blocks)], axis=1)


def expand(z, matrix):
    high, low = halves(z)
    both = dot(jnp.concatenate([high, low], axis=0), matrix)
    return both[: z.shape[0]] + both[z.shape[0] :]


def border_sums(halo, weight, length):
    products = dot(weight, halo)
    out_channels = weight.shape[0] // 9
    width = halo.shape[1]

    def tap(u, v):
        t = 3 * (u + 1) + v + 1
        return products[t * out_channels : (t + 1) * out_channels]

    lane = lanes_of(width)
    part = lane // length
    place = lane % length

    def along(step):
        return jnp.where(
            part == 0,
            tap(-1, step),
            jnp.where(part == 1, tap(1, step), jnp.where(part == 2, tap(step, -1), tap(step, 1))),
        )

    end = 4 * length
    corner = jnp.where(lane == end, tap(-1, -1), 0.0)
    corner = jnp.where(lane == end + 1, tap(-1, 1), corner)
    corner = jnp.where(lane == end + 2, tap(1, -1), corner)
    corner = jnp.where(lane == end + 3, tap(1, 1), corner)
    edge = part < 4
    before = jnp.where(edge & (place != 0), pltpu.roll(along(-1), 1, 1), 0.0)
    after = jnp.where(edge & (place != length - 1), pltpu.roll(along(1), width - 1, 1), 0.0)
    return jnp.where(edge, along(0), corner) + before + after


def with_halo_64(base, halo, weight, west_east, corner_map):
    sums = border_sums(halo, weight, 64)
    rows = sums[:, :128] + expand(sums[:, 256:], corner_map)
    total = base + expand(sums[:, 128:256], west_east)
    cells = total.shape[1]
    low = lanes_of(128) < 64
    top = total[:, :128] + jnp.where(low, rows, 0.0)
    bottom = total[:, cells - 128 :] + jnp.where(low, 0.0, rows)
    return jnp.concatenate([top, total[:, 128 : cells - 128], bottom], axis=1)


def with_halo(base, halo, weight, length, matrix):
    return base + expand(border_sums(halo, weight, length), matrix)


def main_kernel(a_ref, w_ref, out_ref, products, *, length):
    products[...] = dot(w_ref[...], a_ref[...])
    out_channels, cells = out_ref.shape
    lane = lanes_of(cells)
    place = lane % length

    def tap(u, v):
        t = 3 * (u + 1) + v + 1
        return products[t * out_channels : (t + 1) * out_channels, :]

    def column(v):
        above = jnp.where(lane < length, 0.0, pltpu.roll(tap(-1, v), length, 1))
        below = jnp.where(lane >= cells - length, 0.0, pltpu.roll(tap(1, v), cells - length, 1))
        return tap(0, v) + above + below

    total = column(0)
    total += jnp.where(place == 0, 0.0, pltpu.roll(column(-1), 1, 1))
    total += jnp.where(place == length - 1, 0.0, pltpu.roll(column(1), cells - 1, 1))
    out_ref[...] = total


def main_conv(a, weight, length):
    taps_out = weight.shape[0]
    cells = a.shape[1]
    return pl.pallas_call(
        functools.partial(main_kernel, length=length),
        out_shape=jax.ShapeDtypeStruct((taps_out // 9, cells), F32),
        scratch_shapes=[pltpu.VMEM((taps_out, cells), F32)],
        cost_estimate=pl.CostEstimate(
            flops=2 * taps_out * weight.shape[1] * cells * 8, bytes_accessed=a.size * 2 + taps_out * cells, transcendentals=0
        ),
        compiler_params=LIMIT,
        name="main_conv",
    )(in_vmem(a), in_vmem(weight))


def pick_kernel(code_ref, gathered, *outs, specs):
    for target, out in enumerate(outs):
        codes = [code_ref[target * 8 + d] for d in range(8)]
        row_out = 0
        row_in = 0
        for channels, length in specs:
            groups = 64 // length
            rows_in = channels // groups
            lane = lanes_of(128)
            source = lax.broadcasted_iota(jnp.int32, (128, 128), 0) & (2 * length - 1)

            def frame(code):
                rows = gathered[code & 31, row_in : row_in + rows_in, :]
                if groups == 1:
                    return rows
                wide = rows.astype(F32)
                split = [jnp.where(lane // (2 * length) == group, wide, 0.0) for group in range(groups)]
                return jnp.concatenate(split, axis=0).astype(BF16)

            for block in BLOCKS[length]:
                total = None
                for d, base in block:
                    code = codes[d]
                    half = (code >> 5) & 1
                    flip = (code >> 6) & 1
                    active = (code >> 7) == 1
                    start = half * length + flip * (length - 1)
                    if d < 4:
                        cell = start + (1 - 2 * flip) * (lane - base)
                        inside = (lane >= base) & (lane < base + length)
                    else:
                        cell = start + jnp.zeros_like(lane)
                        inside = lane == base
                    cell = jnp.where(inside & active, cell, -1)
                    chosen = jnp.where(source == cell, 1.0, 0.0).astype(BF16)
                    piece = dot(frame(code), chosen)
                    total = piece if total is None else total + piece
                out[row_out : row_out + channels, :] = total.astype(BF16)
                row_out += channels
            row_in += rows_in


def pick(codes, gathered, specs, targets):
    rows = sum(channels * len(BLOCKS[length]) for channels, length in specs)
    shape = jax.ShapeDtypeStruct((rows, 128), BF16)
    return pl.pallas_call(
        functools.partial(pick_kernel, specs=specs),
        out_shape=(shape,) * targets,
        in_specs=[pl.BlockSpec(memory_space=pltpu.SMEM), pl.BlockSpec(memory_space=pltpu.VMEM)],
        compiler_params=LIMIT,
        name="pick",
    )(codes, gathered)


def call(kernel, shapes, *args, name, stage=0):
    return pl.pallas_call(
        kernel,
        out_shape=tuple(jax.ShapeDtypeStruct(s, t) for s, t in shapes),
        scratch_shapes=[pltpu.VMEM((4, stage, 128), BF16)] if stage else [],
        compiler_params=LIMIT,
    )(*(args if name == "start" else [in_vmem(x) for x in args]))


def start_kernel(x_ref, film_ref, a_ref, slots, stage):
    a = activate(x_ref[...].astype(F32), columns_of(film_ref[...]))
    a_ref[...] = a
    put_slots(stage, 0, frame_64(a, ones_at((4096, 128), 1, side_cell)), 64)
    send_slots(stage, slots)


def finish_1(base, x, own, down, up, w, we, cm, wet, c64, x32t, film, skip_ref, a_ref, slots, skip_frame_ref, stage):
    halo = halo_of(own, down, up, 0, 32, 3).astype(BF16)
    first = x[...].astype(F32) + with_halo_64(base[...], halo, w[...], we[...], cm[...])
    skip = first.astype(BF16)
    skip_ref[...] = skip
    a = activate(by_chunks(first, c64[...]), film_of(film, 2))
    a_ref[...] = a
    put_slots(stage, 0, dot(a, x32t[...]).astype(BF16), 32)
    send_slots(stage, slots)
    skip_frame_ref[...] = frame_64(skip, wet[...])


def finish_2(base, own, down, up, w, x32, c32, x32t, x16t, film, skip_ref, a_ref, slots, skip_frame_ref, stage):
    halo = halo_of(own, down, up, 0, 32, 2).astype(BF16)
    second = with_halo(base[...], halo, w[...], 32, x32[...])
    skip = second.astype(BF16)
    skip_ref[...] = skip
    a = activate(by_chunks(second, c32[...]), film_of(film, 3))
    a_ref[...] = a
    put_slots(stage, 0, dot(a, x16t[...]).astype(BF16), 16)
    send_slots(stage, slots)
    skip_frame_ref[...] = dot(skip, x32t[...]).astype(BF16)


def finish_3(base, own, down, up, w, x16, x16t, film, third_ref, a_ref, slots, stage):
    halo = halo_of(own, down, up, 0, 64, 1).astype(BF16)
    third = with_halo(base[...], halo, w[...], 16, x16[...])
    third_ref[...] = third
    a = activate(third, film_of(film, 4))
    a_ref[...] = a
    put_slots(stage, 0, dot(a, x16t[...]).astype(BF16), 16)
    send_slots(stage, slots)


def finish_4(base, third, own, down, up, w, x16, x16t, r32, skip, skip_frame, film, a_ref, slots, stage):
    halo = halo_of(own, down, up, 0, 128, 1).astype(BF16)
    fourth = third[...] + with_halo(base[...], halo, w[...], 16, x16[...])
    put_slots(stage, 0, dot(fourth.astype(BF16), x16t[...]).astype(BF16), 16)
    put_slots(stage, 32, skip_frame[...], 32)
    send_slots(stage, slots)
    joined = jnp.concatenate([by_chunks(fourth, r32[...]), skip[...].astype(F32)], axis=0)
    a_ref[...] = activate(joined, film_of(film, 5))


def finish_5(base, own, down, up, w, x32, x32t, double, r64, skip, skip_frame, film, a_ref, slots, stage):
    coarse = dot(halo_of(own, down, up, 0, 128, 1).astype(BF16), double[...])
    halo = activate(jnp.concatenate([coarse, halo_of(own, down, up, 128, 64, 2)], axis=0), film_of(film, 5))
    fifth = with_halo(base[...], halo, w[...], 32, x32[...])
    put_slots(stage, 0, dot(fifth.astype(BF16), x32t[...]).astype(BF16), 32)
    put_slots(stage, 32, skip_frame[...], 64)
    send_slots(stage, slots)
    joined = jnp.concatenate([by_chunks(fifth, r64[...]), skip[...].astype(F32)], axis=0)
    a_ref[...] = activate(joined, film_of(film, 6))


def finish_6(base, own, down, up, w, we, cm, double, skip, film, out_ref):
    coarse = dot(halo_of(own, down, up, 0, 64, 2).astype(BF16), double[...])
    halo = activate(jnp.concatenate([coarse, halo_of(own, down, up, 128, 32, 3)], axis=0), film_of(film, 6))
    total = with_halo_64(base[...], halo, w[...], we[...], cm[...])
    out_ref[...] = (skip[...].astype(F32) + total).astype(BF16)


def border_cell(k, length):
    cells = length * length
    part, place = k // length, k % length
    cell = jnp.where(part == 0, place, jnp.where(part == 1, cells - length + place, -1))
    cell = jnp.where(part == 2, place * length, jnp.where(part == 3, place * length + length - 1, cell))
    end = 4 * length
    cell = jnp.where(k == end, 0, jnp.where(k == end + 1, length - 1, cell))
    return jnp.where(k == end + 2, cells - length, jnp.where(k == end + 3, cells - 1, cell))


def chunk_lane(lane, length):
    return (lane // length // 2) * (length // 2) + (lane % length) // 2


def double_lane(lane, length):
    end = 4 * length
    half = (lane // length) * (length // 2) + (lane % length) // 2
    return jnp.where(lane < end, half, jnp.where(lane < end + 4, lane - 2 * length, -1))


def side_cell(k):
    return jnp.where(k < 64, k * 64, (k - 64) * 64 + 63)


def corner_lane(k):
    return jnp.where(k == 0, 0, jnp.where(k == 1, 63, jnp.where(k == 2, 64, jnp.where(k == 3, 127, -1))))


def ones_at(shape, axis, function, value=1.0):
    own = [1, 1]
    own[axis] = shape[axis]
    wanted = function(lax.broadcasted_iota(jnp.int32, tuple(own), axis))
    other = lax.broadcasted_iota(jnp.int32, shape, 1 - axis)
    return jnp.where(other == wanted, value, 0.0).astype(BF16)


MATRICES = {
    "we": ((128, 4096), 0, side_cell, 1.0),
    "wet": ((4096, 128), 1, side_cell, 1.0),
    "cm": ((128, 128), 0, corner_lane, 1.0),
    "c64": ((512, 128), 0, lambda k: chunk_lane(k, 64), 0.25),
    "x32t": ((1024, 128), 1, lambda k: border_cell(k, 32), 1.0),
    "x32": ((256, 1024), 0, lambda k: border_cell(k, 32), 1.0),
    "c32": ((512, 128), 0, lambda k: chunk_lane(k, 32), 0.25),
    "x16t": ((256, 128), 1, lambda k: jnp.where(k < 64, border_cell(k, 16), -1), 1.0),
    "x16": ((128, 256), 0, lambda k: border_cell(k, 16), 1.0),
    "r32": ((128, 512), 1, lambda k: chunk_lane(k, 32), 1.0),
    "r64": ((128, 512), 1, lambda k: chunk_lane(k, 64), 1.0),
    "double32": ((128, 256), 1, lambda k: double_lane(k, 32), 1.0),
    "double64": ((256, 384), 1, lambda k: double_lane(k, 64), 1.0),
}


def matrices_kernel(*outs):
    for out, (shape, axis, function, value) in zip(outs, MATRICES.values()):
        out[...] = ones_at(shape, axis, function, value)


def columns_of(film):
    channels = film.shape[1]
    square = [lax.broadcasted_iota(jnp.int32, (channels, channels), dim) for dim in (0, 1)]
    same = square[0] == square[1]
    columns = [jnp.sum(jnp.where(same, film[k : k + 1, :], 0.0), axis=1, keepdims=True) for k in (0, 1)]
    return jnp.concatenate(columns, axis=1)


def prepare_kernel(*refs):
    films, weights, film_out, outs = refs[:6], refs[6:12], refs[12], refs[13:]
    for film, (first, last) in zip(films, FILM_ROWS.values()):
        film_out[first:last, :] = columns_of(film[...])
    for weight, out in zip(weights, outs):
        out_channels = weight.shape[0]
        channels = weight.shape[1] // 9
        for t in range(9):
            out[t * out_channels : (t + 1) * out_channels, :] = weight[:, t * channels : (t + 1) * channels]


def swaps(left):
    pairs = {}
    for one, other in left:
        for a, b in ((one, other), (other, one)):
            pairs[a] = b
            pairs[a // 8 * 8 + 7 - a % 8] = b // 8 * 8 + 7 - b % 8
    return pairs


NEAR_RELAY = {p: p for p in range(32)} | swaps([(1, 11), (8, 10), (16, 18), (25, 19)])
FAR_RELAY = swaps([(0, 24), (2, 26), (3, 27), (1, 19), (25, 11), (8, 18), (16, 10), (9, 17)])


def other_face(face, kind):
    return face ^ 1 if kind == 0 else (face + 1 if face % 2 else face - 1) % 8


def face_moves(kind):
    moves = []
    for face in range(8):
        far = kind == 1 and face % 4 in (0, 3)
        for target, relay in (FAR_RELAY if far else NEAR_RELAY).items():
            moves.append((face * 32 + relay, other_face(face, kind) * 32 + target))
    return moves


def inverse(relays):
    targets = np.full(32, -1)
    for target, relay in relays.items():
        targets[relay] = target
    return targets


def link_codes(link_patch, link_shift, link_turn):
    packed = TURN_EDGE[:, READ_EDGE] * 2 + (TURN_FLIP[:, READ_EDGE] ^ READ_END[None, :])
    choice = jnp.zeros(link_turn.shape, jnp.int32)
    for turn in range(4):
        choice = jnp.where(link_turn == turn, jnp.asarray(packed[turn], jnp.int32), choice)
    edge, flip = choice // 2, choice % 2
    row, column = link_patch // 8, link_patch % 8
    outer = jnp.where(row == 0, 0, jnp.where(row == 3, 1, jnp.where(column == 0, 2, 3)))
    cell_row = jnp.where(edge < 2, edge, flip)
    cell_column = jnp.where(edge < 2, flip, edge - 2)
    in_first = jnp.where(outer < 2, cell_row == outer, cell_column == outer - 2)
    is_corner = jnp.asarray(np.arange(8) >= 4)
    half = jnp.where(is_corner, jnp.where(in_first, 0, 1), jnp.where(edge == outer, 0, 1))
    corner_flip = jnp.where(in_first & (outer < 2), cell_column, cell_row)
    inside = link_shift == 0
    half = jnp.where(inside, 1, half)
    flip = jnp.where(is_corner, jnp.where(inside, cell_column, corner_flip), flip)
    flat = (link_patch + half * 32 + flip * 64 + (link_shift + 1) * 128).reshape(256, 8)
    face = lax.axis_index("face")
    patch = lax.axis_index("patch")
    odd = face % 2
    this = np.arange(32) == patch
    near = jnp.sum(jnp.where(this, jnp.asarray(inverse(NEAR_RELAY), jnp.int32), 0))
    far = jnp.sum(jnp.where(this, jnp.asarray(inverse(FAR_RELAY), jnp.int32), 0))
    far = jnp.where((face % 4 == 0) | (face % 4 == 3), far, near)
    places = [
        (face, patch, 1),
        (face + 1 - 2 * odd, near, 2 * odd),
        ((face + 7 + 2 * odd) % 8, far, 2 - 2 * odd),
    ]
    rows = []
    for of_face, of_patch, shift in places:
        chosen = lax.dynamic_slice(flat, (of_face * 32 + jnp.maximum(of_patch, 0), 0), (1, 8))
        active = (chosen // 128 == shift) & (of_patch >= 0)
        rows.append(chosen % 128 + jnp.where(active, 128, 0))
    return jnp.concatenate(rows, axis=0).reshape(24)


def body(
    features,
    film_first,
    weight_first,
    film_second,
    weight_second,
    film_third,
    weight_third,
    film_fourth,
    weight_fourth,
    film_fifth,
    weight_fifth,
    film_sixth,
    weight_sixth,
    link_patch,
    link_shift,
    link_turn,
):
    x = features[:, 0, :]
    codes = link_codes(link_patch, link_shift, link_turn)
    films = (film_first, film_second, film_third, film_fourth, film_fifth, film_sixth)
    weights = (weight_first, weight_second, weight_third, weight_fourth, weight_fifth, weight_sixth)
    rows = [((9 * w.shape[0], w.shape[1] // 9), BF16) for w in weights]
    film, w1, w2, w3, w4, w5, w6 = call(
        prepare_kernel, [((544, 2), F32)] + rows, *films, *weights, name="prepare"
    )
    made = call(matrices_kernel, [(entry[0], BF16) for entry in MATRICES.values()], name="matrices")
    we, wet, cm, c64, x32t, x32, c32, x16t, x16, r32, r64, double32, double64 = made
    near_moves = face_moves(0)
    far_moves = face_moves(1)

    def exchange(slots, specs):
        gathered = lax.all_to_all(slots, "patch", split_axis=0, concat_axis=0, tiled=True)
        gathered = in_vmem(gathered)
        for_near, for_far = pick(codes[8:], gathered, specs, 2)
        from_far = lax.ppermute(for_far, ("face", "patch"), far_moves)
        from_near = lax.ppermute(for_near, ("face", "patch"), near_moves)
        (own,) = pick(codes[:8], gathered, specs, 1)
        return own, from_near, from_far

    a1, f1 = call(
        start_kernel, [((32, 4096), BF16), ((32, 32, 128), BF16)], x, film_first, name="start", stage=32
    )
    h = exchange(f1, ((32, 64),))
    base = main_conv(a1, w1, 64)
    skip_fine, a2, f2, fine_frame = call(
        finish_1,
        [((32, 4096), BF16), ((32, 1024), BF16), ((32, 16, 128), BF16), ((32, 256), BF16)],
        base, x, *h, w1, we, cm, wet, c64, x32t, film,
        name="finish_1",
        stage=16,
    )
    h = exchange(f2, ((32, 32),))
    base = main_conv(a2, w2, 32)
    skip_middle, a3, f3, middle_frame = call(
        finish_2,
        [((64, 1024), BF16), ((64, 256), BF16), ((32, 16, 128), BF16), ((64, 128), BF16)],
        base, *h, w2, x32, c32, x32t, x16t, film,
        name="finish_2",
        stage=16,
    )
    h = exchange(f3, ((64, 16),))
    base = main_conv(a3, w3, 16)
    third, a4, f4 = call(
        finish_3,
        [((128, 256), F32), ((128, 256), BF16), ((32, 32, 128), BF16)],
        base, *h, w3, x16, x16t, film,
        name="finish_3",
        stage=32,
    )
    h = exchange(f4, ((128, 16),))
    base = main_conv(a4, w4, 16)
    a5, f5 = call(
        finish_4,
        [((192, 1024), BF16), ((32, 64, 128), BF16)],
        base, third, *h, w4, x16, x16t, r32, skip_middle, middle_frame, film,
        name="finish_4",
        stage=64,
    )
    h = exchange(f5, ((128, 16), (64, 32)))
    base = main_conv(a5, w5, 32)
    a6, f6 = call(
        finish_5,
        [((96, 4096), BF16), ((32, 64, 128), BF16)],
        base, *h, w5, x32, x32t, double32, r64, skip_fine, fine_frame, film,
        name="finish_5",
        stage=64,
    )
    h = exchange(f6, ((64, 32), (32, 64)))
    base = main_conv(a6, w6, 64)
    (result,) = call(
        finish_6,
        [((32, 4096), BF16)],
        base, *h, w6, we, cm, double64, skip_fine, film,
        name="finish_6",
    )
    return result[:, None, :]


def solution(mesh):
    in_specs = (P(None, "face", "patch"),) + (P(),) * 15
    out_specs = P(None, "face", "patch")
    return jax.shard_map(body, mesh=mesh, in_specs=in_specs, out_specs=out_specs, check_vma=False)
```
